32 devices in a mesh: dp: 2 (over x), yz: 4 (over z), x: 4 (over y, core).
Axes of the slice: x: 2, y: 2, z: 4, core: 2. Of those that a mesh axis runs over, the one named last changes fastest.
Arguments:
- x_in: bfloat16 [128, 4096], P('dp', ('x', 'yz')), parts along dimension 0
- ln_gain: bfloat16 [4096], P(('x', 'yz'))
- w_qkv: bfloat16 [4096, 4608], P('x', 'yz')
- w_gate: bfloat16 [4096, 16384], P('x', 'yz')
- w_up: bfloat16 [4096, 16384], P('x', 'yz')
- w_attn_out: bfloat16 [4096, 4096], P('yz', 'x')
- w_mlp_out: bfloat16 [16384, 4096], P('yz', 'x')
- k_cache: bfloat16 [128, 4096, 256], P(('dp', 'x', 'yz')), parts along dimension 0
- v_cache: bfloat16 [128, 4096, 256], P(('dp', 'x', 'yz')), parts along dimension 0
- ctx_len: int32 [128], P(('dp', 'x', 'yz')), parts along dimension 0
Outputs:
- output 1: bfloat16 [128, 4096], P('dp', ('x', 'yz')), parts along dimension 0
- output 2: bfloat16 [128, 4096, 256], P(('dp', 'x', 'yz')), parts along dimension 0
- output 3: bfloat16 [128, 4096, 256], P(('dp', 'x', 'yz')), parts along dimension 0
There are 2 independent parts. The reference program is written for one: setup_inputs(seed, part) draws one part's arguments, and reference() takes and returns one part's arrays. A program takes and returns all parts, laid end to end along the dimension named above; an argument that names none is the same for every part.
All inputs are finite; a program needn't handle non-finite values.
Results may differ from the reference program's by a relative error of at most 0.00713757.
Values are sent between devices in bfloat16 or wider.
A program may use at most 1 GiB of HBM per device.

```python
import jax
import jax.numpy as jnp
from jax import lax

BATCH_SIZE = 64
D_MODEL = 4096
NUM_HEADS = 16
HEAD_DIM = 256
FF_DIM = 16384
CACHE_LEN = 4096


def setup_inputs(seed: int = 0, part: int = 0) -> dict:
    part_key = jax.random.fold_in(jax.random.key(seed), part)
    shared_key = jax.random.key(seed + 1)
    x_key, kc_key, vc_key, vm_key, len_key = jax.random.split(part_key, 5)
    g_key, qkv_key, gate_key, up_key, ao_key, mo_key = jax.random.split(shared_key, 6)
    qkv_cols = (NUM_HEADS + 2) * HEAD_DIM
    attn_cols = NUM_HEADS * HEAD_DIM
    x_in = jax.random.normal(x_key, (BATCH_SIZE, D_MODEL), jnp.float32)
    ln_gain = jax.random.uniform(g_key, (D_MODEL,), jnp.float32, 0.5, 1.5)
    w_qkv = jax.random.normal(qkv_key, (D_MODEL, qkv_cols), jnp.float32) * D_MODEL ** -0.5
    w_gate = jax.random.normal(gate_key, (D_MODEL, FF_DIM), jnp.float32) * D_MODEL ** -0.5
    w_up = jax.random.normal(up_key, (D_MODEL, FF_DIM), jnp.float32) * D_MODEL ** -0.5
    w_attn_out = jax.random.normal(ao_key, (attn_cols, D_MODEL), jnp.float32) * attn_cols ** -0.5
    w_mlp_out = jax.random.normal(mo_key, (FF_DIM, D_MODEL), jnp.float32) * FF_DIM ** -0.5
    k_cache = jax.random.normal(kc_key, (BATCH_SIZE, CACHE_LEN, HEAD_DIM), jnp.float32)
    v_mean = jax.random.normal(vm_key, (BATCH_SIZE, 1, HEAD_DIM), jnp.float32)
    v_cache = v_mean + 0.7 * jax.random.normal(vc_key, (BATCH_SIZE, CACHE_LEN, HEAD_DIM), jnp.float32)
    ctx_len = jax.random.randint(len_key, (BATCH_SIZE,), CACHE_LEN // 8, CACHE_LEN, jnp.int32)
    ctx_len = ctx_len.at[0].set(CACHE_LEN - 1).at[1].set(CACHE_LEN // 8)
    return {
        "x_in": x_in.astype(jnp.bfloat16),
        "ln_gain": ln_gain.astype(jnp.bfloat16),
        "w_qkv": w_qkv.astype(jnp.bfloat16),
        "w_gate": w_gate.astype(jnp.bfloat16),
        "w_up": w_up.astype(jnp.bfloat16),
        "w_attn_out": w_attn_out.astype(jnp.bfloat16),
        "w_mlp_out": w_mlp_out.astype(jnp.bfloat16),
        "k_cache": k_cache.astype(jnp.bfloat16),
        "v_cache": v_cache.astype(jnp.bfloat16),
        "ctx_len": ctx_len,
    }


def apply_rope(vecs, positions):
    half_dim = vecs.shape[-1] // 2
    inv_freq = 10000.0 ** (-jnp.arange(half_dim, dtype=jnp.float32) / half_dim)
    angles = positions.astype(jnp.float32)[..., None] * inv_freq
    cos_t = jnp.cos(angles)
    sin_t = jnp.sin(angles)
    first_half = vecs[..., :half_dim]
    second_half = vecs[..., half_dim:]
    return jnp.concatenate([first_half * cos_t - second_half * sin_t, second_half * cos_t + first_half * sin_t], axis=-1)


def layer_norm(x_in, ln_gain):
    x_f32 = x_in.astype(jnp.float32)
    row_mean = jnp.sum(x_f32, axis=-1, keepdims=True) / D_MODEL
    row_var = jnp.sum(x_f32 * x_f32, axis=-1, keepdims=True) / D_MODEL - row_mean * row_mean
    normed = (x_f32 - row_mean) * lax.rsqrt(row_var + 1e-6) * ln_gain.astype(jnp.float32)
    return normed.astype(jnp.bfloat16)


def reference(x_in, ln_gain, w_qkv, w_gate, w_up, w_attn_out, w_mlp_out, k_cache, v_cache, ctx_len):
    normed = layer_norm(x_in, ln_gain)
    qkv_proj = jnp.dot(normed, w_qkv, preferred_element_type=jnp.float32).astype(jnp.bfloat16)
    gate_proj = jnp.dot(normed, w_gate, preferred_element_type=jnp.float32).astype(jnp.bfloat16)
    up_proj = jnp.dot(normed, w_up, preferred_element_type=jnp.float32).astype(jnp.bfloat16)
    mlp_act = (jax.nn.silu(gate_proj.astype(jnp.float32)) * up_proj.astype(jnp.float32)).astype(jnp.bfloat16)
    attn_cols = NUM_HEADS * HEAD_DIM
    q_heads = qkv_proj[:, :attn_cols].reshape(BATCH_SIZE, NUM_HEADS, HEAD_DIM)
    k_new = qkv_proj[:, attn_cols:attn_cols + HEAD_DIM]
    v_new = qkv_proj[:, attn_cols + HEAD_DIM:]
    q_rot = apply_rope(q_heads.astype(jnp.float32), ctx_len[:, None]).astype(jnp.bfloat16)
    k_rot = apply_rope(k_new.astype(jnp.float32), ctx_len).astype(jnp.bfloat16)
    positions = jnp.arange(CACHE_LEN)
    new_slot = (positions[None, :] == ctx_len[:, None])[:, :, None]
    k_out = jnp.where(new_slot, k_rot[:, None, :], k_cache)
    v_out = jnp.where(new_slot, v_new[:, None, :], v_cache)
    block_rows = 8
    n_blocks = BATCH_SIZE // block_rows

    def attend(block_in):
        q_blk, k_blk, v_blk, len_blk = block_in
        scores = jnp.einsum("bhd,btd->bht", q_blk.astype(jnp.float32), k_blk.astype(jnp.float32)) * HEAD_DIM ** -0.5
        visible = (positions[None, :] <= len_blk[:, None])[:, None, :]
        scores = jnp.where(visible, scores, -1e30)
        attn_probs = jax.nn.softmax(scores, axis=-1).astype(jnp.bfloat16)
        return jnp.einsum("bht,btd->bhd", attn_probs.astype(jnp.float32), v_blk.astype(jnp.float32)).astype(jnp.bfloat16)

    attn_heads = lax.map(attend, (
        q_rot.reshape(n_blocks, block_rows, NUM_HEADS, HEAD_DIM),
        k_out.reshape(n_blocks, block_rows, CACHE_LEN, HEAD_DIM),
        v_out.reshape(n_blocks, block_rows, CACHE_LEN, HEAD_DIM),
        ctx_len.reshape(n_blocks, block_rows),
    ))
    attn_flat = attn_heads.reshape(BATCH_SIZE, attn_cols)
    z_sum = jnp.dot(attn_flat, w_attn_out, preferred_element_type=jnp.float32) + jnp.dot(mlp_act, w_mlp_out, preferred_element_type=jnp.float32)
    y_out = (x_in.astype(jnp.float32) + z_sum).astype(jnp.bfloat16)
    return (y_out, k_out, v_out)
```

```python
import jax
import jax.numpy as jnp
from jax import lax
from jax.sharding import PartitionSpec as P
from jax.experimental import pallas as pl
from jax.experimental.pallas import tpu as pltpu

MESH = pl.DeviceIdType.MESH
F32 = jnp.float32
BF16 = jnp.bfloat16

LN_X, LN_S, QKV_D, QKV_Y, Q_Z = 0, 3, 6, 8, 9
GU_0, GU_Y, GU_2 = 12, 16, 20
A_D, A_Y, A_F = 24, 28, 32
O_Z, O_X, Z_R = 36, 39, 42
N_SEM = 45


def dot(a, b):
    return jnp.dot(a, b, preferred_element_type=F32)


def layer_kernel(x_ref, g_ref, cos_ref, sin_ref, len_ref, wqkv, wg, wu, wao, wmo, kc, vc,
                 y_ref, ko, vo,
                 wqkv_v, wg_v, wu_v, wao_v, wmo_v,
                 xg, st, h_ref, qp, qr, qys, qy, zs, zr, qa, qb, kn, vn, s_ref, osa, osb,
                 gs0, r1, ys, yr, gs2, r3, p3, a_all, oz, orr, o_all, z_buf, z_rec,
                 lsem, ssem, rsem):
    i = lax.axis_index("x")
    j = lax.axis_index("yz")
    n_rows = x_ref.shape[0]
    d_model = 16 * x_ref.shape[1]

    def rc(src, dst, k, **dev):
        return pltpu.make_async_remote_copy(src_ref=src, dst_ref=dst, send_sem=ssem.at[k], recv_sem=rsem.at[k],
                                            device_id=dev, device_id_type=MESH)

    loads = [pltpu.make_async_copy(wqkv, wqkv_v, lsem.at[0])]
    for s in range(4):
        cols = pl.ds(pl.multiple_of((i ^ (3 - s)) * 1024, 1024), 1024)
        loads.append(pltpu.make_async_copy(wg.at[:, cols], wg_v.at[s], lsem.at[1 + 2 * s]))
        loads.append(pltpu.make_async_copy(wu.at[:, cols], wu_v.at[s], lsem.at[2 + 2 * s]))
    kv_loads = []
    for r in range(4):
        kv_loads.append(pltpu.make_async_copy(kc.at[r], ko.at[r], lsem.at[9 + 2 * r]))
        kv_loads.append(pltpu.make_async_copy(vc.at[r], vo.at[r], lsem.at[10 + 2 * r]))
    w_loads = [pltpu.make_async_copy(wmo, wmo_v, lsem.at[17]), pltpu.make_async_copy(wao, wao_v, lsem.at[18])]
    for c in loads + kv_loads + w_loads:
        c.start()

    barrier = pltpu.get_barrier_semaphore()
    for d in (1, 2, 3):
        pl.semaphore_signal(barrier, inc=1, device_id={"yz": j ^ d}, device_id_type=MESH)
        pl.semaphore_signal(barrier, inc=1, device_id={"x": i ^ d}, device_id_type=MESH)
    xg.at[j][0:64, :] = x_ref[...]
    xg.at[j][64:80, :] = jnp.broadcast_to(g_ref[...], (16, 256))
    pl.semaphore_wait(barrier, 6)

    ln = [rc(xg.at[j], xg.at[j], LN_X + d - 1, yz=j ^ d) for d in (1, 2, 3)]
    for c in ln:
        c.start()
    for c in ln:
        c.wait()
    acc1 = jnp.zeros((64, 256), F32)
    acc2 = jnp.zeros((64, 256), F32)
    for jj in range(4):
        xb = xg[jj, 0:64, :].astype(F32)
        acc1 += xb
        acc2 += xb * xb
    s1 = jnp.sum(acc1, axis=1, keepdims=True)
    s2 = jnp.sum(acc2, axis=1, keepdims=True)
    lane = lax.broadcasted_iota(jnp.int32, (64, 128), 1)
    stat = jnp.where(lane == 0, s1, jnp.where(lane == 1, s2, 0.0))
    st.at[i][...] = jnp.concatenate([stat, jnp.zeros((64, 128), F32)], axis=0).T[0:8, :]
    sts = [rc(st.at[i], st.at[i], LN_S + d - 1, x=i ^ d) for d in (1, 2, 3)]
    for c in sts:
        c.start()
    for c in sts:
        c.wait()
    tot = (st[0] + st[1]) + (st[2] + st[3])
    tot = jnp.concatenate([tot, jnp.zeros((120, 128), F32)], axis=0).T
    mean = tot[0:64, 0:1] / d_model
    var = tot[0:64, 1:2] / d_model - mean * mean
    rstd = lax.rsqrt(var + 1e-6)
    for jj in range(4):
        xb = xg[jj, 0:64, :].astype(F32)
        gb = xg[jj, 64:80, :].astype(F32)[0:1, :]
        h_ref[:, jj * 256:(jj + 1) * 256] = ((xb - mean) * rstd * gb).astype(BF16)

    loads[0].wait()
    for n in range(3):
        cols = slice(n * 384, (n + 1) * 384)
        part = dot(h_ref[...], wqkv_v[:, cols])
        for b in range(4):
            qp[b, :, cols] = part[b * 16:(b + 1) * 16, :]
    qd = [rc(qp.at[i ^ 3], qr.at[0], QKV_D, x=i ^ 1), rc(qp.at[i ^ 1], qr.at[1], QKV_D + 1, x=i ^ 1)]
    for c in qd:
        c.start()

    def gu_part(s, q):
        cols = pl.ds(pl.multiple_of(q * 256, 256), 256)
        hv = h_ref[...]
        return dot(hv, wg_v[s, :, cols]), dot(hv, wu_v[s, :, cols])

    def c0(q):
        return rc(gs0.at[q], r1.at[q], GU_0 + q, x=i ^ 1)

    def cy(q):
        return rc(ys.at[q], yr.at[q], GU_Y + q, x=i ^ 2)

    def c2(q):
        return rc(gs2.at[q], r3.at[q], GU_2 + q, x=i ^ 1)

    loads[1].wait()
    loads[2].wait()

    def slot0(q, _):
        g, u = gu_part(0, q)
        gs0[q, 0] = g
        gs0[q, 1] = u
        c0(q).start()
        return 0

    lax.fori_loop(0, 4, slot0, 0)
    for c in qd:
        c.wait()
    qys[...] = qp[i ^ 2] + qr[0]
    qyc = rc(qys, qy, QKV_Y, x=i ^ 2)
    qyc.start()
    loads[3].wait()
    loads[4].wait()

    def slot1(q, _):
        g, u = gu_part(1, q)
        c0(q).wait()
        ys[q, 0] = g + r1[q, 0]
        ys[q, 1] = u + r1[q, 1]
        cy(q).start()
        return 0

    lax.fori_loop(0, 4, slot1, 0)
    loads[5].wait()
    loads[6].wait()

    def slot2(q, _):
        g, u = gu_part(2, q)
        gs2[q, 0] = g
        gs2[q, 1] = u
        c2(q).start()
        return 0

    lax.fori_loop(0, 4, slot2, 0)

    qyc.wait()
    fin = ((qp[i] + qr[1]) + qy[...]).astype(BF16).astype(F32)
    for b in range(4):
        zs[b] = fin[b * 4:(b + 1) * 4, :]
    qz = [rc(zs.at[j ^ d], zr.at[j], Q_Z + d - 1, yz=j ^ d) for d in (1, 2, 3)]
    for c in qz:
        c.start()
    zr.at[j][...] = zs[j]
    loads[7].wait()
    loads[8].wait()

    def slot3(q, _):
        g, u = gu_part(3, q)
        p3[q, 0] = g
        p3[q, 1] = u
        return 0

    lax.fori_loop(0, 4, slot3, 0)
    for c in qz:
        c.wait()

    cos_t = cos_ref[...]
    sin_t = sin_ref[...]

    def half(k):
        return zr[k // 9, :, (k % 9) * 128:(k % 9 + 1) * 128]

    def rope(k):
        u1, u2 = half(k), half(k + 1)
        return ((u1 * cos_t - u2 * sin_t).astype(BF16).astype(F32), (u2 * cos_t + u1 * sin_t).astype(BF16).astype(F32))

    for hd in range(16):
        t1, t2 = rope(2 * hd)
        qa[hd * 8:hd * 8 + 4, :] = t1
        qb[hd * 8:hd * 8 + 4, :] = t2
    t1, t2 = rope(32)
    kn[0:4, 0:128] = t1
    kn[0:4, 128:256] = t2
    vn[0:4, 0:128] = half(34)
    vn[0:4, 128:256] = half(35)
    for c in kv_loads:
        c.wait()

    def ca(q):
        return rc(a_all.at[i * 4 + q], a_all.at[i * 4 + q], A_D + q, x=i ^ 1)

    def cay(q):
        return rc(a_all.at[i * 4 + q], a_all.at[i * 4 + q], A_Y + q, x=i ^ 2)

    def request(r, _):
        q_r = jnp.concatenate([qa[pl.ds(r, 16, stride=8), :], qb[pl.ds(r, 16, stride=8), :]], axis=1)
        k_new = kn[pl.ds(r, 1), :]
        v_new = vn[pl.ds(r, 1), :]
        pos_r = len_ref[r]
        s_new = jnp.sum(q_r * k_new, axis=1, keepdims=True) * 0.0625
        qb16 = q_r.astype(BF16)
        for t in range(4):
            sc = lax.dot_general(qb16, ko[r, t * 1024:(t + 1) * 1024, :], (((1,), (1,)), ((), ())),
                                 preferred_element_type=F32) * 0.0625
            pos = t * 1024 + lax.broadcasted_iota(jnp.int32, (16, 1024), 1)
            s_ref[:, t * 1024:(t + 1) * 1024] = jnp.where(pos < pos_r, sc, -1e30)
        sc = s_ref[...]
        top = jnp.maximum(jnp.max(sc, axis=1, keepdims=True), s_new)
        e = jnp.exp(sc - top)
        e_new = jnp.exp(s_new - top)
        inv = 1.0 / (jnp.sum(e, axis=1, keepdims=True) + e_new)
        o = (e_new * inv).astype(BF16).astype(F32) * v_new
        o = o + dot((e * inv).astype(BF16), vo[r])
        o = o.astype(BF16).astype(F32)
        rows = pl.ds(pl.multiple_of(r * 16, 16), 16)
        osa[rows, :] = o[:, 0:128]
        osb[rows, :] = o[:, 128:256]
        q = r
        c2(q).wait()
        cy(q).wait()
        g = ((p3[q, 0] + r3[q, 0]) + yr[q, 0]).astype(BF16).astype(F32)
        u = ((p3[q, 1] + r3[q, 1]) + yr[q, 1]).astype(BF16).astype(F32)
        a_all.at[i * 4 + q][...] = (g * jax.nn.sigmoid(g) * u).astype(BF16)
        ca(q).start()
        cay(q).start()
        return 0

    lax.fori_loop(0, 4, request, 0)

    for b in range(4):
        for hh in range(4):
            hd = b * 4 + hh
            oz[b, hh, :, 0:128] = osa[pl.ds(hd, 4, stride=16), :]
            oz[b, hh, :, 128:256] = osb[pl.ds(hd, 4, stride=16), :]
    ozc = [rc(oz.at[j ^ d], orr.at[j], O_Z + d - 1, yz=j ^ d) for d in (1, 2, 3)]
    for c in ozc:
        c.start()
    orr.at[j][...] = oz[j]

    w_loads[0].wait()
    z_buf[...] = jnp.zeros_like(z_buf)

    def z_add(k):
        av = a_all[k]
        rows = pl.ds(pl.multiple_of(k * 256, 256), 256)
        for n in range(4):
            z_buf[n] += dot(av, wmo_v[rows, n * 256:(n + 1) * 256])

    def z_own(q, _):
        z_add(i * 4 + q)
        return 0

    lax.fori_loop(0, 4, z_own, 0)
    for c in ozc:
        c.wait()
    for hh in range(4):
        o_all.at[i][hh] = jnp.concatenate([orr[b, hh] for b in range(4)], axis=0).astype(BF16)
    oxc = [rc(o_all.at[i], o_all.at[i], O_X + d - 1, x=i ^ d) for d in (1, 2, 3)]
    for c in oxc:
        c.start()

    def cf(q):
        k = (i ^ 2) * 4 + q
        return rc(a_all.at[k], a_all.at[k], A_F + q, x=i ^ 1)

    def z_partner(q, _):
        ca(q).wait()
        z_add((i ^ 1) * 4 + q)
        return 0

    def z_far(q, _):
        cay(q).wait()
        cf(q).start()
        z_add((i ^ 2) * 4 + q)
        return 0

    def z_fwd(q, _):
        cf(q).wait()
        z_add((i ^ 3) * 4 + q)
        return 0

    lax.fori_loop(0, 4, z_partner, 0)
    lax.fori_loop(0, 4, z_far, 0)
    lax.fori_loop(0, 4, z_fwd, 0)

    for c in oxc:
        c.wait()
    w_loads[1].wait()
    ov = [jnp.concatenate([o_all[b, hh] for b in range(4)], axis=0) for hh in range(4)]
    ov = jnp.concatenate(ov, axis=1)
    for n in range(4):
        z_buf[n] += dot(ov, wao_v[:, n * 256:(n + 1) * 256])
    zc = [rc(z_buf.at[j ^ d], z_rec.at[d - 1], Z_R + d - 1, yz=j ^ d) for d in (3, 2, 1)]
    for c in zc:
        c.start()

    def insert(r, _):
        k_new = kn[pl.ds(r, 1), :].astype(BF16)
        v_new = vn[pl.ds(r, 1), :].astype(BF16)
        pos_r = len_ref[r]

        def chunk(t, _):
            rows = pl.ds(pl.multiple_of(t * 256, 256), 256)
            pos = t * 256 + lax.broadcasted_iota(jnp.int32, (256, 256), 0)
            ko[r, rows, :] = jnp.where(pos == pos_r, k_new, ko[r, rows, :])
            vo[r, rows, :] = jnp.where(pos == pos_r, v_new, vo[r, rows, :])
            return 0

        return lax.fori_loop(0, 16, chunk, 0)

    lax.fori_loop(0, 4, insert, 0)

    for c in zc:
        c.wait()
    z = (z_buf[j] + z_rec[0]) + (z_rec[1] + z_rec[2])
    y_ref[...] = (x_ref[...].astype(F32) + z).astype(BF16)


def solution(mesh):
    both_axes = ("x", "yz")
    row_spec = P("dp", both_axes)
    in_w_spec = P("x", "yz")
    out_w_spec = P("yz", "x")
    cache_spec = P(("dp", "x", "yz"), None, None)
    len_spec = P(("dp", "x", "yz"))

    def local_layer(x_loc, gain_loc, wqkv, wg, wu, wao, wmo, kc, vc, len_loc):
        half_dim = kc.shape[2] // 2
        inv_freq = 10000.0 ** (-jnp.arange(half_dim, dtype=F32) / half_dim)
        angles = len_loc.astype(F32)[:, None] * inv_freq
        vm = pl.BlockSpec(memory_space=pltpu.VMEM)
        hbm = pl.BlockSpec(memory_space=pl.ANY)
        gu = pltpu.VMEM((4, 2, 64, 256), F32)
        y, ko, vo = pl.pallas_call(
            layer_kernel,
            out_shape=(jax.ShapeDtypeStruct(x_loc.shape, BF16), pltpu.VMEM(kc.shape, BF16), pltpu.VMEM(vc.shape, BF16)),
            in_specs=[vm] * 4 + [pl.BlockSpec(memory_space=pltpu.SMEM)] + [hbm] * 7,
            out_specs=(vm, vm, vm),
            scratch_shapes=[
                pltpu.VMEM((1024, 1152), BF16), pltpu.VMEM((4, 1024, 1024), BF16), pltpu.VMEM((4, 1024, 1024), BF16),
                pltpu.VMEM((1024, 1024), BF16), pltpu.VMEM((4096, 1024), BF16),
                pltpu.VMEM((4, 80, 256), BF16), pltpu.VMEM((4, 8, 128), F32), pltpu.VMEM((64, 1024), BF16),
                pltpu.VMEM((4, 16, 1152), F32), pltpu.VMEM((2, 16, 1152), F32), pltpu.VMEM((16, 1152), F32),
                pltpu.VMEM((16, 1152), F32), pltpu.VMEM((4, 4, 1152), F32), pltpu.VMEM((4, 4, 1152), F32),
                pltpu.VMEM((128, 128), F32), pltpu.VMEM((128, 128), F32), pltpu.VMEM((8, 256), F32),
                pltpu.VMEM((8, 256), F32), pltpu.VMEM((16, 4096), F32), pltpu.VMEM((64, 128), F32),
                pltpu.VMEM((64, 128), F32),
                gu, gu, gu, gu, gu, gu, gu,
                pltpu.VMEM((16, 64, 256), BF16), pltpu.VMEM((4, 4, 4, 256), F32), pltpu.VMEM((4, 4, 4, 256), F32),
                pltpu.VMEM((4, 4, 16, 256), BF16), pltpu.VMEM((4, 64, 256), F32), pltpu.VMEM((3, 64, 256), F32),
                pltpu.SemaphoreType.DMA((19,)), pltpu.SemaphoreType.DMA((N_SEM,)), pltpu.SemaphoreType.DMA((N_SEM,)),
            ],
            compiler_params=pltpu.CompilerParams(collective_id=0, has_side_effects=True,
                                                 vmem_limit_bytes=46 * 1024 * 1024),
        )(x_loc, gain_loc.reshape(1, -1), jnp.cos(angles), jnp.sin(angles), len_loc, wqkv, wg, wu, wao, wmo, kc, vc)
        return y, ko, vo

    in_specs = (row_spec, P(both_axes), in_w_spec, in_w_spec, in_w_spec, out_w_spec, out_w_spec, cache_spec, cache_spec, len_spec)
    out_specs = (row_spec, cache_spec, cache_spec)
    return jax.shard_map(local_layer, mesh=mesh, in_specs=in_specs, out_specs=out_specs, check_vma=False)
```

```python
import jax
import numpy as np
import jax.numpy as jnp
from jax import lax
from jax.sharding import PartitionSpec as P
from jax.experimental import pallas as pl
from jax.experimental.pallas import tpu as pltpu

MESH = pl.DeviceIdType.MESH
F32 = jnp.float32
BF16 = jnp.bfloat16

LN_X, LN_S, QKV_D, QKV_Y, Q_Z = 0, 3, 18, 20, 21
GU_0, GU_Y, GU_2 = 24, 28, 32
A_D, A_Y, A_F = 36, 40, 44
O_Z, O_X, Z_R = 48, 51, 54
N_SEM = 57


def dot(a, b):
    return jnp.dot(a, b, preferred_element_type=F32)


def layer_kernel(x_hbm, g_ref, freq_ref, len_ref, wqkv, wg, wu, wao, wmo, kc, vc,
                 y_ref, ko, vo,
                 wqkv_v, wg_v, wu_v, wao_v, wmo_v,
                 xg, st, cs, h_ref, qp, qr, qys, qy, zs, zr, qa, qb, kn, vn, s_ref, osa, osb,
                 gs0, r1, ys, yr, gs2, r3, p3, a_all, oz, orr, o_all, z_buf, z_rec,
                 lsem, ssem, rsem):
    i = lax.axis_index("x")
    j = lax.axis_index("yz")
    d_model = 16 * x_hbm.shape[1]

    def rc(src, dst, k, **dev):
        return pltpu.make_async_remote_copy(src_ref=src, dst_ref=dst, send_sem=ssem.at[k], recv_sem=rsem.at[k],
                                            device_id=dev, device_id_type=MESH)

    barrier = pltpu.get_barrier_semaphore()
    group = [(d & 3, d >> 2) for d in range(1, 16)]
    for dx, dz in group:
        pl.semaphore_signal(barrier, inc=1, device_id={"x": i ^ dx, "yz": j ^ dz}, device_id_type=MESH)
    x_load = pltpu.make_async_copy(x_hbm, xg.at[j, pl.ds(0, 64)], lsem.at[19])
    x_load.start()
    loads = [pltpu.make_async_copy(wqkv, wqkv_v, lsem.at[0])]
    for s in range(4):
        cols = pl.ds(pl.multiple_of((i ^ (3 - s)) * 1024, 1024), 1024)
        loads.append(pltpu.make_async_copy(wg.at[:, cols], wg_v.at[s], lsem.at[1 + 2 * s]))
        loads.append(pltpu.make_async_copy(wu.at[:, cols], wu_v.at[s], lsem.at[2 + 2 * s]))
    kv_loads = []
    for r in range(4):
        kv_loads.append(pltpu.make_async_copy(kc.at[r], ko.at[r], lsem.at[9 + 2 * r]))
        kv_loads.append(pltpu.make_async_copy(vc.at[r], vo.at[r], lsem.at[10 + 2 * r]))
    w_loads = [pltpu.make_async_copy(wmo, wmo_v, lsem.at[17]), pltpu.make_async_copy(wao, wao_v, lsem.at[18])]
    for c in loads:
        c.start()

    xg.at[j][64:80, :] = jnp.broadcast_to(g_ref[...].reshape(1, 256), (16, 256))
    x_load.wait()
    xf = xg.at[j][0:64, :].astype(F32)
    s1 = jnp.sum(xf, axis=1, keepdims=True)
    s2 = jnp.sum(xf * xf, axis=1, keepdims=True)
    lane = lax.broadcasted_iota(jnp.int32, (64, 128), 1)
    stat = jnp.where(lane == 0, s1, jnp.where(lane == 1, s2, 0.0))
    me = j * 4 + i
    st.at[me][...] = jnp.concatenate([stat, jnp.zeros((64, 128), F32)], axis=0).T[0:8, :]
    pl.semaphore_wait(barrier, 15)

    ln = [rc(xg.at[j], xg.at[j], LN_X + d - 1, yz=j ^ d) for d in (3, 2, 1)]
    for n, (dx, dz) in enumerate(group):
        ln.append(rc(st.at[me], st.at[me], LN_S + n, x=i ^ dx, yz=j ^ dz))
    for c in ln:
        c.start()
    for c in kv_loads + w_loads:
        c.start()
    row = lax.broadcasted_iota(jnp.int32, (4, 128), 0)
    pos = jnp.zeros((4, 128), F32)
    for r in range(4):
        pos = jnp.where(row == r, len_ref[r].astype(F32), pos)
    angle = pos * freq_ref[...]
    cs[0] = jnp.cos(angle)
    cs[1] = jnp.sin(angle)
    for c in ln:
        c.wait()
    tot = st[0]
    for n in range(1, 16):
        tot = tot + st[n]
    tot = jnp.concatenate([tot, jnp.zeros((120, 128), F32)], axis=0).T
    mean = tot[0:64, 0:1] / d_model
    var = tot[0:64, 1:2] / d_model - mean * mean
    rstd = lax.rsqrt(var + 1e-6)
    for jj in range(4):
        xb = xg[jj, 0:64, :].astype(F32)
        gb = xg[jj, 64:80, :].astype(F32)[0:1, :]
        h_ref[:, jj * 256:(jj + 1) * 256] = ((xb - mean) * rstd * gb).astype(BF16)

    loads[0].wait()
    for n in range(3):
        cols = slice(n * 384, (n + 1) * 384)
        part = dot(h_ref[...], wqkv_v[:, cols])
        for b in range(4):
            qp[b, :, cols] = part[b * 16:(b + 1) * 16, :]
    qd = [rc(qp.at[i ^ 3], qr.at[0], QKV_D, x=i ^ 1), rc(qp.at[i ^ 1], qr.at[1], QKV_D + 1, x=i ^ 1)]
    for c in qd:
        c.start()

    def gu_part(s, q):
        cols = pl.ds(pl.multiple_of(q * 256, 256), 256)
        hv = h_ref[...]
        return dot(hv, wg_v[s, :, cols]), dot(hv, wu_v[s, :, cols])

    def c0(q):
        return rc(gs0.at[q], r1.at[q], GU_0 + q, x=i ^ 1)

    def cy(q):
        return rc(ys.at[q], yr.at[q], GU_Y + q, x=i ^ 2)

    def c2(q):
        return rc(gs2.at[q], r3.at[q], GU_2 + q, x=i ^ 1)

    loads[1].wait()
    loads[2].wait()

    def slot0(q, _):
        g, u = gu_part(0, q)
        gs0[q, 0] = g
        gs0[q, 1] = u
        c0(q).start()
        return 0

    lax.fori_loop(0, 4, slot0, 0)
    for c in qd:
        c.wait()
    qys[...] = qp[i ^ 2] + qr[0]
    qyc = rc(qys, qy, QKV_Y, x=i ^ 2)
    qyc.start()
    loads[3].wait()
    loads[4].wait()

    def slot1(q, _):
        g, u = gu_part(1, q)
        c0(q).wait()
        ys[q, 0] = g + r1[q, 0]
        ys[q, 1] = u + r1[q, 1]
        cy(q).start()
        return 0

    lax.fori_loop(0, 4, slot1, 0)
    loads[5].wait()
    loads[6].wait()

    def slot2(q, _):
        g, u = gu_part(2, q)
        gs2[q, 0] = g
        gs2[q, 1] = u
        c2(q).start()
        return 0

    lax.fori_loop(0, 4, slot2, 0)

    qyc.wait()
    fin = ((qp[i] + qr[1]) + qy[...]).astype(BF16)
    for b in range(4):
        zs[b] = fin[b * 4:(b + 1) * 4, :]
    qz = [rc(zs.at[j ^ d], zr.at[j], Q_Z + d - 1, yz=j ^ d) for d in (1, 2, 3)]
    for c in qz:
        c.start()
    zr.at[j][...] = zs[j]
    loads[7].wait()
    loads[8].wait()

    def slot3(q, _):
        g, u = gu_part(3, q)
        p3[q, 0] = g
        p3[q, 1] = u
        return 0

    lax.fori_loop(0, 4, slot3, 0)
    for c in qz:
        c.wait()

    cos_t = cs[0]
    sin_t = cs[1]

    def half(k):
        return zr[k // 9, :, (k % 9) * 128:(k % 9 + 1) * 128].astype(F32)

    def rope(k):
        u1, u2 = half(k), half(k + 1)
        return ((u1 * cos_t - u2 * sin_t).astype(BF16).astype(F32), (u2 * cos_t + u1 * sin_t).astype(BF16).astype(F32))

    for hd in range(16):
        t1, t2 = rope(2 * hd)
        qa[hd * 8:hd * 8 + 4, :] = t1
        qb[hd * 8:hd * 8 + 4, :] = t2
    t1, t2 = rope(32)
    kn[0:4, 0:128] = t1
    kn[0:4, 128:256] = t2
    vn[0:4, 0:128] = half(34)
    vn[0:4, 128:256] = half(35)
    for c in kv_loads:
        c.wait()

    def ca(q):
        return rc(a_all.at[i * 4 + q], a_all.at[i * 4 + q], A_D + q, x=i ^ 1)

    def cay(q):
        return rc(a_all.at[i * 4 + q], a_all.at[i * 4 + q], A_Y + q, x=i ^ 2)

    def request(r):
        q_r = jnp.concatenate([qa[pl.ds(r, 16, stride=8), :], qb[pl.ds(r, 16, stride=8), :]], axis=1)
        k_new = kn[r:r + 1, :]
        v_new = vn[r:r + 1, :]
        pos_r = len_ref[r]
        s_new = jnp.sum(q_r * k_new, axis=1, keepdims=True) * 0.0625
        qb16 = q_r.astype(BF16)
        for t in range(4):
            sc = lax.dot_general(qb16, ko[r, t * 1024:(t + 1) * 1024, :], (((1,), (1,)), ((), ())),
                                 preferred_element_type=F32) * 0.0625
            pos = t * 1024 + lax.broadcasted_iota(jnp.int32, (16, 1024), 1)
            s_ref[r, :, t * 1024:(t + 1) * 1024] = jnp.where(pos < pos_r, sc, -1e30)
        sc = s_ref[r]
        top = jnp.maximum(jnp.max(sc, axis=1, keepdims=True), s_new)
        e = jnp.exp(sc - top)
        e_new = jnp.exp(s_new - top)
        inv = 1.0 / (jnp.sum(e, axis=1, keepdims=True) + e_new)
        o = (e_new * inv).astype(BF16).astype(F32) * v_new
        o = o + dot((e * inv).astype(BF16), vo[r])
        o = o.astype(BF16).astype(F32)
        osa[r * 16:(r + 1) * 16, :] = o[:, 0:128]
        osb[r * 16:(r + 1) * 16, :] = o[:, 128:256]

    def activation(q):
        c2(q).wait()
        cy(q).wait()
        g = ((p3[q, 0] + r3[q, 0]) + yr[q, 0]).astype(BF16).astype(F32)
        u = ((p3[q, 1] + r3[q, 1]) + yr[q, 1]).astype(BF16).astype(F32)
        a_all.at[i * 4 + q][...] = (g * jax.nn.sigmoid(g) * u).astype(BF16)
        ca(q).start()
        cay(q).start()

    request(0)
    request(1)
    activation(0)
    activation(1)
    request(2)
    request(3)

    for b in range(4):
        for hh in range(4):
            hd = b * 4 + hh
            oz[b, hh, :, 0:128] = osa[pl.ds(hd, 4, stride=16), :]
            oz[b, hh, :, 128:256] = osb[pl.ds(hd, 4, stride=16), :]
    ozc = [rc(oz.at[j ^ d], orr.at[j], O_Z + d - 1, yz=j ^ d) for d in (3, 2, 1)]
    for c in ozc:
        c.start()
    orr.at[j][...] = oz[j]
    activation(2)
    activation(3)

    w_loads[0].wait()
    z_buf[...] = jnp.zeros_like(z_buf)

    def z_add(k):
        av = a_all[k]
        rows = pl.ds(pl.multiple_of(k * 256, 256), 256)
        for n in range(4):
            z_buf[n] += dot(av, wmo_v[rows, n * 256:(n + 1) * 256])

    def z_own(q, _):
        z_add(i * 4 + q)
        return 0

    def cf(q):
        k = (i ^ 2) * 4 + q
        return rc(a_all.at[k], a_all.at[k], A_F + q, x=i ^ 1)

    def z_partner(q, _):
        ca(q).wait()
        z_add((i ^ 1) * 4 + q)
        return 0

    def z_far(q, _):
        cay(q).wait()
        cf(q).start()
        z_add((i ^ 2) * 4 + q)
        return 0

    def z_fwd(q, _):
        cf(q).wait()
        z_add((i ^ 3) * 4 + q)
        return 0

    lax.fori_loop(0, 4, z_own, 0)
    for c in ozc:
        c.wait()
    for hh in range(4):
        o_all.at[i][hh] = jnp.concatenate([orr[b, hh] for b in range(4)], axis=0).astype(BF16)
    oxc = [rc(o_all.at[i], o_all.at[i], O_X + d - 1, x=i ^ d) for d in (2, 3, 1)]
    for c in oxc:
        c.start()

    lax.fori_loop(0, 4, z_partner, 0)
    lax.fori_loop(0, 4, z_far, 0)
    lax.fori_loop(0, 4, z_fwd, 0)

    for c in oxc:
        c.wait()
    w_loads[1].wait()
    ov = [jnp.concatenate([o_all[b, hh] for b in range(4)], axis=0) for hh in range(4)]
    ov = jnp.concatenate(ov, axis=1)
    zc = []
    for d in (3, 2, 1, 0):
        cols = pl.ds(pl.multiple_of((j ^ d) * 256, 256), 256)
        z_buf.at[j ^ d][...] += dot(ov, wao_v[:, cols])
        if d:
            zc.append(rc(z_buf.at[j ^ d], z_rec.at[d - 1], Z_R + d - 1, yz=j ^ d))
            zc[-1].start()

    def insert(r, _):
        k_new = kn[pl.ds(r, 1), :].astype(BF16)
        v_new = vn[pl.ds(r, 1), :].astype(BF16)
        pos_r = len_ref[r]

        def chunk(t, _):
            rows = pl.ds(pl.multiple_of(t * 256, 256), 256)
            pos = t * 256 + lax.broadcasted_iota(jnp.int32, (256, 256), 0)
            ko[r, rows, :] = jnp.where(pos == pos_r, k_new, ko[r, rows, :])
            vo[r, rows, :] = jnp.where(pos == pos_r, v_new, vo[r, rows, :])
            return 0

        return lax.fori_loop(0, 16, chunk, 0)

    lax.fori_loop(0, 4, insert, 0)

    for c in zc:
        c.wait()
    z = (z_buf[j] + z_rec[0]) + (z_rec[1] + z_rec[2])
    y_ref[...] = (xg.at[j][0:64, :].astype(F32) + z).astype(BF16)


def solution(mesh):
    both_axes = ("x", "yz")
    row_spec = P("dp", both_axes)
    in_w_spec = P("x", "yz")
    out_w_spec = P("yz", "x")
    cache_spec = P(("dp", "x", "yz"), None, None)
    len_spec = P(("dp", "x", "yz"))

    def local_layer(x_loc, gain_loc, wqkv, wg, wu, wao, wmo, kc, vc, len_loc):
        half_dim = kc.shape[2] // 2
        inv_freq = np.float32(10000.0) ** (-np.arange(half_dim, dtype=np.float32) / np.float32(half_dim))
        vm = pl.BlockSpec(memory_space=pltpu.VMEM)
        hbm = pl.BlockSpec(memory_space=pl.ANY)
        gu = pltpu.VMEM((4, 2, 64, 256), F32)
        y, ko, vo = pl.pallas_call(
            layer_kernel,
            out_shape=(pltpu.VMEM(x_loc.shape, BF16), pltpu.VMEM(kc.shape, BF16), pltpu.VMEM(vc.shape, BF16)),
            in_specs=[hbm, vm, vm] + [pl.BlockSpec(memory_space=pltpu.SMEM)] + [hbm] * 7,
            out_specs=(vm, vm, vm),
            scratch_shapes=[
                pltpu.VMEM((1024, 1152), BF16), pltpu.VMEM((4, 1024, 1024), BF16), pltpu.VMEM((4, 1024, 1024), BF16),
                pltpu.VMEM((1024, 1024), BF16), pltpu.VMEM((4096, 1024), BF16),
                pltpu.VMEM((4, 80, 256), BF16), pltpu.VMEM((16, 8, 128), F32), pltpu.VMEM((2, 4, 128), F32),
                pltpu.VMEM((64, 1024), BF16),
                pltpu.VMEM((4, 16, 1152), F32), pltpu.VMEM((2, 16, 1152), F32), pltpu.VMEM((16, 1152), F32),
                pltpu.VMEM((16, 1152), F32), pltpu.VMEM((4, 4, 1152), BF16), pltpu.VMEM((4, 4, 1152), BF16),
                pltpu.VMEM((128, 128), F32), pltpu.VMEM((128, 128), F32), pltpu.VMEM((8, 256), F32),
                pltpu.VMEM((8, 256), F32), pltpu.VMEM((4, 16, 4096), F32), pltpu.VMEM((64, 128), F32),
                pltpu.VMEM((64, 128), F32),
                gu, gu, gu, gu, gu, gu, gu,
                pltpu.VMEM((16, 64, 256), BF16), pltpu.VMEM((4, 4, 4, 256), F32), pltpu.VMEM((4, 4, 4, 256), F32),
                pltpu.VMEM((4, 4, 16, 256), BF16), pltpu.VMEM((4, 64, 256), F32), pltpu.VMEM((3, 64, 256), F32),
                pltpu.SemaphoreType.DMA((20,)), pltpu.SemaphoreType.DMA((N_SEM,)), pltpu.SemaphoreType.DMA((N_SEM,)),
            ],
            compiler_params=pltpu.CompilerParams(collective_id=0, has_side_effects=True,
                                                 vmem_limit_bytes=46 * 1024 * 1024),
        )(x_loc, gain_loc, inv_freq.reshape(1, -1), len_loc, wqkv, wg, wu, wao, wmo, kc, vc)
        return y, ko, vo

    in_specs = (row_spec, P(both_axes), in_w_spec, in_w_spec, in_w_spec, out_w_spec, out_w_spec, cache_spec, cache_spec, len_spec)
    out_specs = (row_spec, cache_spec, cache_spec)
    return jax.shard_map(local_layer, mesh=mesh, in_specs=in_specs, out_specs=out_specs, check_vma=False)
```

```python
import jax
import numpy as np
import jax.numpy as jnp
from jax import lax
from jax.sharding import PartitionSpec as P
from jax.experimental import pallas as pl
from jax.experimental.pallas import tpu as pltpu

MESH = pl.DeviceIdType.MESH
F32 = jnp.float32
BF16 = jnp.bfloat16

LN_X, LN_G, LN_S, LN_Z, QKV_D, QKV_Y, Q_Z = 0, 3, 6, 9, 12, 14, 15
GU_0, GU_Y, GU_2 = 18, 22, 26
A_D, A_Y, A_F = 30, 34, 38
O_Z, O_X, Z_R = 42, 45, 48
N_SEM = 51


def dot(a, b):
    return jnp.dot(a, b, preferred_element_type=F32)


def layer_kernel(x_hbm, g_ref, freq_ref, len_ref, wqkv, wg, wu, wao, wmo, kc, vc,
                 y_ref, ko, vo,
                 wqkv_v, wg_v, wu_v, wao_v, wmo_v,
                 xg, gs, st, sz, cs, h_ref, qp, qr, qys, qy, zs, zr, qa, qb, kn, vn, s_ref, osa, osb,
                 gs0, r1, ys, yr, gs2, r3, p3, a_all, oz, orr, o_all, z_buf, z_rec,
                 lsem, ssem, rsem):
    i = lax.axis_index("x")
    j = lax.axis_index("yz")
    d_model = 16 * x_hbm.shape[1]

    def rc(src, dst, k, **dev):
        return pltpu.make_async_remote_copy(src_ref=src, dst_ref=dst, send_sem=ssem.at[k], recv_sem=rsem.at[k],
                                            device_id=dev, device_id_type=MESH)

    barrier = pltpu.get_barrier_semaphore()
    for d in (3, 2, 1):
        pl.semaphore_signal(barrier, inc=1, device_id={"yz": j ^ d}, device_id_type=MESH)
        pl.semaphore_signal(barrier, inc=1, device_id={"x": i ^ d}, device_id_type=MESH)
    x_load = pltpu.make_async_copy(x_hbm, xg.at[j], lsem.at[19])
    x_load.start()
    loads = [pltpu.make_async_copy(wqkv, wqkv_v, lsem.at[0])]
    for s in range(4):
        cols = pl.ds(pl.multiple_of((i ^ (3 - s)) * 1024, 1024), 1024)
        loads.append(pltpu.make_async_copy(wg.at[:, cols], wg_v.at[s], lsem.at[1 + 2 * s]))
        loads.append(pltpu.make_async_copy(wu.at[:, cols], wu_v.at[s], lsem.at[2 + 2 * s]))
    kv_loads = []
    for r in range(4):
        kv_loads.append(pltpu.make_async_copy(kc.at[r], ko.at[r], lsem.at[9 + 2 * r]))
        kv_loads.append(pltpu.make_async_copy(vc.at[r], vo.at[r], lsem.at[10 + 2 * r]))
    w_loads = [pltpu.make_async_copy(wmo, wmo_v, lsem.at[17]), pltpu.make_async_copy(wao, wao_v, lsem.at[18])]
    for c in loads:
        c.start()

    gs.at[j][...] = g_ref[...].reshape(1, 256).astype(F32)
    x_load.wait()
    xf = xg[j].astype(F32)
    s1 = jnp.sum(xf, axis=1, keepdims=True)
    s2 = jnp.sum(xf * xf, axis=1, keepdims=True)
    stat = jnp.broadcast_to(jnp.concatenate([s1, s2], axis=0), (128, 128))
    st.at[i][...] = stat.T[0:1, :]
    pl.semaphore_wait(barrier, 6)

    lns = [rc(st.at[i], st.at[i], LN_S + d - 1, x=i ^ d) for d in (3, 2, 1)]
    ln = [rc(xg.at[j], xg.at[j], LN_X + d - 1, yz=j ^ d) for d in (3, 2, 1)]
    ln += [rc(gs.at[j], gs.at[j], LN_G + d - 1, yz=j ^ d) for d in (3, 2, 1)]
    for c in lns + ln:
        c.start()
    for c in lns:
        c.wait()
    sz.at[j][...] = (st[0] + st[1]) + (st[2] + st[3])
    lnz = [rc(sz.at[j], sz.at[j], LN_Z + d - 1, yz=j ^ d) for d in (3, 2, 1)]
    for c in lnz:
        c.start()
    for c in kv_loads + w_loads:
        c.start()
    row = lax.broadcasted_iota(jnp.int32, (4, 128), 0)
    pos = jnp.zeros((4, 128), F32)
    for r in range(4):
        pos = jnp.where(row == r, len_ref[r].astype(F32), pos)
    angle = pos * freq_ref[...]
    cs[0] = jnp.cos(angle)
    cs[1] = jnp.sin(angle)
    for c in lnz:
        c.wait()
    for c in ln:
        c.wait()
    tot = jnp.broadcast_to((sz[0] + sz[1]) + (sz[2] + sz[3]), (128, 128)).T
    mean = tot[0:64, 0:1] / d_model
    var = tot[64:128, 0:1] / d_model - mean * mean
    rstd = lax.rsqrt(var + 1e-6)
    for jj in range(4):
        xb = xg[jj].astype(F32)
        h_ref[:, jj * 256:(jj + 1) * 256] = ((xb - mean) * rstd * gs[jj]).astype(BF16)

    loads[0].wait()
    for n in range(3):
        cols = slice(n * 384, (n + 1) * 384)
        part = dot(h_ref[...], wqkv_v[:, cols])
        for b in range(4):
            qp[b, :, cols] = part[b * 16:(b + 1) * 16, :]
    qd = [rc(qp.at[i ^ 3], qr.at[0], QKV_D, x=i ^ 1), rc(qp.at[i ^ 1], qr.at[1], QKV_D + 1, x=i ^ 1)]
    for c in qd:
        c.start()

    def gu_part(s, q):
        cols = pl.ds(pl.multiple_of(q * 256, 256), 256)
        hv = h_ref[...]
        return dot(hv, wg_v[s, :, cols]), dot(hv, wu_v[s, :, cols])

    def c0(q):
        return rc(gs0.at[q], r1.at[q], GU_0 + q, x=i ^ 1)

    def cy(q):
        return rc(ys.at[q], yr.at[q], GU_Y + q, x=i ^ 2)

    def c2(q):
        return rc(gs2.at[q], r3.at[q], GU_2 + q, x=i ^ 1)

    loads[1].wait()
    loads[2].wait()

    def slot0(q, _):
        g, u = gu_part(0, q)
        gs0[q, 0] = g
        gs0[q, 1] = u
        c0(q).start()
        return 0

    lax.fori_loop(0, 4, slot0, 0)
    for c in qd:
        c.wait()
    qys[...] = qp[i ^ 2] + qr[0]
    qyc = rc(qys, qy, QKV_Y, x=i ^ 2)
    qyc.start()
    loads[3].wait()
    loads[4].wait()

    def slot1(q, _):
        g, u = gu_part(1, q)
        c0(q).wait()
        ys[q, 0] = g + r1[q, 0]
        ys[q, 1] = u + r1[q, 1]
        cy(q).start()
        return 0

    lax.fori_loop(0, 4, slot1, 0)
    loads[5].wait()
    loads[6].wait()

    def slot2(q, _):
        g, u = gu_part(2, q)
        gs2[q, 0] = g
        gs2[q, 1] = u
        c2(q).start()
        return 0

    lax.fori_loop(0, 4, slot2, 0)

    qyc.wait()
    fin = ((qp[i] + qr[1]) + qy[...]).astype(BF16)
    for b in range(4):
        zs[b] = fin[b * 4:(b + 1) * 4, :]
    qz = [rc(zs.at[j ^ d], zr.at[j], Q_Z + d - 1, yz=j ^ d) for d in (1, 2, 3)]
    for c in qz:
        c.start()
    zr.at[j][...] = zs[j]
    loads[7].wait()
    loads[8].wait()

    def slot3(q, _):
        g, u = gu_part(3, q)
        p3[q, 0] = g
        p3[q, 1] = u
        return 0

    lax.fori_loop(0, 4, slot3, 0)
    for c in qz:
        c.wait()

    cos_t = cs[0]
    sin_t = cs[1]

    def half(k):
        return zr[k // 9, :, (k % 9) * 128:(k % 9 + 1) * 128].astype(F32)

    def rope(k):
        u1, u2 = half(k), half(k + 1)
        return ((u1 * cos_t - u2 * sin_t).astype(BF16).astype(F32), (u2 * cos_t + u1 * sin_t).astype(BF16).astype(F32))

    for hd in range(16):
        t1, t2 = rope(2 * hd)
        qa[hd * 8:hd * 8 + 4, :] = t1
        qb[hd * 8:hd * 8 + 4, :] = t2
    t1, t2 = rope(32)
    kn[0:4, 0:128] = t1
    kn[0:4, 128:256] = t2
    vn[0:4, 0:128] = half(34)
    vn[0:4, 128:256] = half(35)
    for c in kv_loads:
        c.wait()

    def ca(q):
        return rc(a_all.at[i * 4 + q], a_all.at[i * 4 + q], A_D + q, x=i ^ 1)

    def cay(q):
        return rc(a_all.at[i * 4 + q], a_all.at[i * 4 + q], A_Y + q, x=i ^ 2)

    def request(r):
        q_r = jnp.concatenate([qa[pl.ds(r, 16, stride=8), :], qb[pl.ds(r, 16, stride=8), :]], axis=1)
        k_new = kn[r:r + 1, :]
        v_new = vn[r:r + 1, :]
        pos_r = len_ref[r]
        s_new = jnp.sum(q_r * k_new, axis=1, keepdims=True) * 0.0625
        qb16 = q_r.astype(BF16)
        for t in range(4):
            sc = lax.dot_general(qb16, ko[r, t * 1024:(t + 1) * 1024, :], (((1,), (1,)), ((), ())),
                                 preferred_element_type=F32) * 0.0625
            pos = t * 1024 + lax.broadcasted_iota(jnp.int32, (16, 1024), 1)
            s_ref[r, :, t * 1024:(t + 1) * 1024] = jnp.where(pos < pos_r, sc, -1e30)
        sc = s_ref[r]
        top = jnp.maximum(jnp.max(sc, axis=1, keepdims=True), s_new)
        e = jnp.exp(sc - top)
        e_new = jnp.exp(s_new - top)
        inv = 1.0 / (jnp.sum(e, axis=1, keepdims=True) + e_new)
        o = (e_new * inv).astype(BF16).astype(F32) * v_new
        o = o + dot((e * inv).astype(BF16), vo[r])
        o = o.astype(BF16).astype(F32)
        osa[r * 16:(r + 1) * 16, :] = o[:, 0:128]
        osb[r * 16:(r + 1) * 16, :] = o[:, 128:256]

    def activation(q):
        c2(q).wait()
        cy(q).wait()
        g = ((p3[q, 0] + r3[q, 0]) + yr[q, 0]).astype(BF16).astype(F32)
        u = ((p3[q, 1] + r3[q, 1]) + yr[q, 1]).astype(BF16).astype(F32)
        a_all.at[i * 4 + q][...] = (g * jax.nn.sigmoid(g) * u).astype(BF16)
        ca(q).start()
        cay(q).start()

    for r in range(4):
        request(r)

    for b in range(4):
        for hh in range(4):
            hd = b * 4 + hh
            oz[b, hh, :, 0:128] = osa[pl.ds(hd, 4, stride=16), :].astype(BF16)
            oz[b, hh, :, 128:256] = osb[pl.ds(hd, 4, stride=16), :].astype(BF16)
    ozc = [rc(oz.at[j ^ d], orr.at[j], O_Z + d - 1, yz=j ^ d) for d in (3, 2, 1)]
    for c in ozc:
        c.start()
    orr.at[j][...] = oz[j]
    activation(0)
    activation(1)
    activation(2)
    activation(3)

    w_loads[0].wait()
    z_buf[...] = jnp.zeros_like(z_buf)

    def z_add(k):
        av = a_all[k]
        rows = pl.ds(pl.multiple_of(k * 256, 256), 256)
        for n in range(4):
            z_buf[n] += dot(av, wmo_v[rows, n * 256:(n + 1) * 256])

    def z_own(q, _):
        z_add(i * 4 + q)
        return 0

    def cf(q):
        k = (i ^ 2) * 4 + q
        return rc(a_all.at[k], a_all.at[k], A_F + q, x=i ^ 1)

    def z_partner(q, _):
        ca(q).wait()
        z_add((i ^ 1) * 4 + q)
        return 0

    def z_far(q, _):
        cay(q).wait()
        cf(q).start()
        z_add((i ^ 2) * 4 + q)
        return 0

    def z_fwd(q, _):
        cf(q).wait()
        z_add((i ^ 3) * 4 + q)
        return 0

    lax.fori_loop(0, 4, z_own, 0)
    for c in ozc:
        c.wait()
    for hh in range(4):
        o_all.at[i][hh] = jnp.concatenate([orr[b, hh].astype(F32) for b in range(4)], axis=0).astype(BF16)
    oxc = [rc(o_all.at[i], o_all.at[i], O_X + d - 1, x=i ^ d) for d in (2, 3, 1)]
    for c in oxc:
        c.start()

    lax.fori_loop(0, 4, z_far, 0)
    lax.fori_loop(0, 4, z_partner, 0)
    lax.fori_loop(0, 4, z_fwd, 0)

    for c in oxc:
        c.wait()
    w_loads[1].wait()
    ov = [jnp.concatenate([o_all[b, hh] for b in range(4)], axis=0) for hh in range(4)]
    ov = jnp.concatenate(ov, axis=1)
    zc = []
    for d in (3, 2, 1, 0):
        cols = pl.ds(pl.multiple_of((j ^ d) * 256, 256), 256)
        z_buf.at[j ^ d][...] += dot(ov, wao_v[:, cols])
        if d:
            zc.append(rc(z_buf.at[j ^ d], z_rec.at[d - 1], Z_R + d - 1, yz=j ^ d))
            zc[-1].start()

    def insert(r, _):
        k_new = kn[pl.ds(r, 1), :].astype(BF16)
        v_new = vn[pl.ds(r, 1), :].astype(BF16)
        pos_r = len_ref[r]

        def chunk(t, _):
            rows = pl.ds(pl.multiple_of(t * 256, 256), 256)
            pos = t * 256 + lax.broadcasted_iota(jnp.int32, (256, 256), 0)
            ko[r, rows, :] = jnp.where(pos == pos_r, k_new, ko[r, rows, :])
            vo[r, rows, :] = jnp.where(pos == pos_r, v_new, vo[r, rows, :])
            return 0

        return lax.fori_loop(0, 16, chunk, 0)

    lax.fori_loop(0, 4, insert, 0)

    for c in zc:
        c.wait()
    z = (z_buf[j] + z_rec[0]) + (z_rec[1] + z_rec[2])
    y_ref[...] = (xg[j].astype(F32) + z).astype(BF16)


def write_kernel(y_in, ki, vi, y_out, ko, vo, sem):
    copies = [pltpu.make_async_copy(y_in, y_out, sem.at[16])]
    for r in range(4):
        for b in range(2):
            rows = pl.ds(b * 2048, 2048)
            copies.append(pltpu.make_async_copy(ki.at[r, rows], ko.at[r, rows], sem.at[r * 4 + b]))
            copies.append(pltpu.make_async_copy(vi.at[r, rows], vo.at[r, rows], sem.at[r * 4 + b + 2]))
    for c in copies:
        c.start()
    for c in copies:
        c.wait()


def solution(mesh):
    both_axes = ("x", "yz")
    row_spec = P("dp", both_axes)
    in_w_spec = P("x", "yz")
    out_w_spec = P("yz", "x")
    cache_spec = P(("dp", "x", "yz"), None, None)
    len_spec = P(("dp", "x", "yz"))

    def local_layer(x_loc, gain_loc, wqkv, wg, wu, wao, wmo, kc, vc, len_loc):
        half_dim = kc.shape[2] // 2
        inv_freq = np.float32(10000.0) ** (-np.arange(half_dim, dtype=np.float32) / np.float32(half_dim))
        vm = pl.BlockSpec(memory_space=pltpu.VMEM)
        hbm = pl.BlockSpec(memory_space=pl.ANY)
        gu = pltpu.VMEM((4, 2, 64, 256), F32)
        y, ko, vo = pl.pallas_call(
            layer_kernel, name="layer",
            out_shape=(pltpu.VMEM(x_loc.shape, BF16), pltpu.VMEM(kc.shape, BF16), pltpu.VMEM(vc.shape, BF16)),
            in_specs=[hbm, vm, vm] + [pl.BlockSpec(memory_space=pltpu.SMEM)] + [hbm] * 7,
            out_specs=(vm, vm, vm),
            scratch_shapes=[
                pltpu.VMEM((1024, 1152), BF16), pltpu.VMEM((4, 1024, 1024), BF16), pltpu.VMEM((4, 1024, 1024), BF16),
                pltpu.VMEM((1024, 1024), BF16), pltpu.VMEM((4096, 1024), BF16),
                pltpu.VMEM((4, 64, 256), BF16), pltpu.VMEM((4, 1, 256), F32),
                pltpu.VMEM((4, 1, 128), F32), pltpu.VMEM((4, 1, 128), F32), pltpu.VMEM((2, 4, 128), F32),
                pltpu.VMEM((64, 1024), BF16),
                pltpu.VMEM((4, 16, 1152), F32), pltpu.VMEM((2, 16, 1152), F32), pltpu.VMEM((16, 1152), F32),
                pltpu.VMEM((16, 1152), F32), pltpu.VMEM((4, 4, 1152), BF16), pltpu.VMEM((4, 4, 1152), BF16),
                pltpu.VMEM((128, 128), F32), pltpu.VMEM((128, 128), F32), pltpu.VMEM((8, 256), F32),
                pltpu.VMEM((8, 256), F32), pltpu.VMEM((4, 16, 4096), F32), pltpu.VMEM((64, 128), F32),
                pltpu.VMEM((64, 128), F32),
                gu, gu, gu, gu, gu, gu, gu,
                pltpu.VMEM((16, 64, 256), BF16), pltpu.VMEM((4, 4, 4, 256), BF16), pltpu.VMEM((4, 4, 4, 256), BF16),
                pltpu.VMEM((4, 4, 16, 256), BF16), pltpu.VMEM((4, 64, 256), F32), pltpu.VMEM((3, 64, 256), F32),
                pltpu.SemaphoreType.DMA((20,)), pltpu.SemaphoreType.DMA((N_SEM,)), pltpu.SemaphoreType.DMA((N_SEM,)),
            ],
            compiler_params=pltpu.CompilerParams(collective_id=0, has_side_effects=True,
                                                 vmem_limit_bytes=46 * 1024 * 1024),
        )(x_loc, gain_loc, inv_freq.reshape(1, -1), len_loc, wqkv, wg, wu, wao, wmo, kc, vc)
        return pl.pallas_call(
            write_kernel, name="write",
            out_shape=tuple(jax.ShapeDtypeStruct(a.shape, BF16) for a in (x_loc, kc, vc)),
            in_specs=[vm] * 3,
            out_specs=[hbm] * 3,
            scratch_shapes=[pltpu.SemaphoreType.DMA((17,))],
            compiler_params=pltpu.CompilerParams(vmem_limit_bytes=8 * 1024 * 1024),
        )(y, ko, vo)

    in_specs = (row_spec, P(both_axes), in_w_spec, in_w_spec, in_w_spec, out_w_spec, out_w_spec, cache_spec, cache_spec, len_spec)
    out_specs = (row_spec, cache_spec, cache_spec)
    return jax.shard_map(local_layer, mesh=mesh, in_specs=in_specs, out_specs=out_specs, check_vma=False)
```

```python
import jax
import numpy as np
import jax.numpy as jnp
from jax import lax
from jax.sharding import PartitionSpec as P
from jax.experimental import pallas as pl
from jax.experimental.pallas import tpu as pltpu

MESH = pl.DeviceIdType.MESH
F32 = jnp.float32
BF16 = jnp.bfloat16

S_LX, S_LG, S_LS, S_LZ, S_QD, S_QY, S_QZ, S_G0, S_GY, S_G2, S_AD, S_AY, S_AF, S_OZ, S_OX, S_Z = range(16)
N_SEND = 16
R_LX, R_LG, R_LS, R_LZ, R_Q0, R_Q1, R_QY, R_QZ, R_G0, R_GY, R_G2, R_AD, R_AY, R_AF, R_OZ, R_OX, R_Z = (
    0, 1, 2, 3, 4, 7, 8, 9, 10, 14, 18, 19, 20, 24, 26, 27, 28)
N_RECV = 29
L_X, L_QKV, L_GU, L_K, L_V, L_MO, L_AO, L_S = 0, 1, 2, 6, 7, 8, 9, 10
N_LOAD = 13


def dot(a, b):
    return jnp.dot(a, b, preferred_element_type=F32)


def layer_kernel(x_hbm, g_hbm, freq_hbm, len_hbm, wqkv, wg, wu, wao, wmo, kc, vc,
                 y_ref, ko, vo,
                 g_v, freq_v, len_ref, wqkv_v, wg_v, wu_v, wao_v, wmo_v,
                 xg, gs, st, sz, cs, h_ref, qp, qr, qys, qy, zs, zr, qa, qb, kn, vn, s_ref, osa, osb,
                 gs0, r1, ys, yr, gs2, r3, p3, a_all, oz, orr, o_all, z_buf, z_rec,
                 lsem, ssem, rsem):
    i = lax.axis_index("x")
    j = lax.axis_index("yz")
    d_model = 16 * x_hbm.shape[1]
    away = (3, 2, 1)

    def rc(src, dst, s, r, **dev):
        return pltpu.make_async_remote_copy(src_ref=src, dst_ref=dst, send_sem=ssem.at[s], recv_sem=rsem.at[r],
                                            device_id=dev, device_id_type=MESH)

    def start(copies):
        for c in copies:
            c.start()

    def arrived(ref, r):
        rc(ref, ref, 0, r, x=i ^ 1).wait_recv()

    def sent(ref, s):
        rc(ref, ref, s, 0, x=i ^ 1).wait_send()

    barrier = pltpu.get_barrier_semaphore()
    for d in away:
        pl.semaphore_signal(barrier, inc=1, device_id={"yz": j ^ d}, device_id_type=MESH)
        pl.semaphore_signal(barrier, inc=1, device_id={"x": i ^ d}, device_id_type=MESH)
    small = [pltpu.make_async_copy(x_hbm, xg.at[j], lsem.at[L_X]),
             pltpu.make_async_copy(g_hbm, g_v, lsem.at[L_S]),
             pltpu.make_async_copy(freq_hbm, freq_v, lsem.at[L_S + 1]),
             pltpu.make_async_copy(len_hbm, len_ref, lsem.at[L_S + 2])]
    start(small)
    qkv_load = pltpu.make_async_copy(wqkv, wqkv_v, lsem.at[L_QKV])
    qkv_load.start()
    for s in range(4):
        cols = pl.ds(pl.multiple_of((i ^ (3 - s)) * 1024, 1024), 1024)
        pltpu.make_async_copy(wg.at[:, cols], wg_v.at[s], lsem.at[L_GU + s]).start()
        pltpu.make_async_copy(wu.at[:, cols], wu_v.at[s], lsem.at[L_GU + s]).start()

    def gu_loaded(s):
        pltpu.make_async_copy(wg_v.at[0:2], wg_v.at[0:2], lsem.at[L_GU + s]).wait()

    later = [pltpu.make_async_copy(kc, ko, lsem.at[L_K]), pltpu.make_async_copy(vc, vo, lsem.at[L_V]),
             pltpu.make_async_copy(wmo, wmo_v, lsem.at[L_MO]), pltpu.make_async_copy(wao, wao_v, lsem.at[L_AO])]

    for c in small:
        c.wait()
    gs.at[j][...] = g_v[...].reshape(1, 256).astype(F32)
    xf = xg[j].astype(F32)
    s1 = jnp.sum(xf, axis=1, keepdims=True)
    s2 = jnp.sum(xf * xf, axis=1, keepdims=True)
    stat = jnp.broadcast_to(jnp.concatenate([s1, s2], axis=0), (128, 128))
    st.at[i][...] = stat.T[0:1, :]
    pl.semaphore_wait(barrier, 6)

    start([rc(st.at[i], st.at[i], S_LS, R_LS, x=i ^ d) for d in away])
    start([rc(xg.at[j], xg.at[j], S_LX, R_LX, yz=j ^ d) for d in away])
    start([rc(gs.at[j], gs.at[j], S_LG, R_LG, yz=j ^ d) for d in away])
    arrived(st.at[0:3], R_LS)
    sz.at[j][...] = (st[0] + st[1]) + (st[2] + st[3])
    start([rc(sz.at[j], sz.at[j], S_LZ, R_LZ, yz=j ^ d) for d in away])
    start(later)
    row = lax.broadcasted_iota(jnp.int32, (4, 128), 0)
    pos = jnp.zeros((4, 128), F32)
    for r in range(4):
        pos = jnp.where(row == r, len_ref[r].astype(F32), pos)
    angle = pos * freq_v[...]
    cs[0] = jnp.cos(angle)
    cs[1] = jnp.sin(angle)
    arrived(sz.at[0:3], R_LZ)
    arrived(gs.at[0:3], R_LG)
    arrived(xg.at[0:3], R_LX)
    tot = jnp.broadcast_to((sz[0] + sz[1]) + (sz[2] + sz[3]), (128, 128)).T
    mean = tot[0:64, 0:1] / d_model
    var = tot[64:128, 0:1] / d_model - mean * mean
    rstd = lax.rsqrt(var + 1e-6)
    for jj in range(4):
        xb = xg[jj].astype(F32)
        h_ref[:, jj * 256:(jj + 1) * 256] = ((xb - mean) * rstd * gs[jj]).astype(BF16)

    qkv_load.wait()
    for n in range(3):
        part = dot(h_ref[...], wqkv_v[:, n * 384:(n + 1) * 384])
        for b in range(4):
            qp[n, b] = part[b * 16:(b + 1) * 16, :]
        rc(qp.at[n, i ^ 3], qr.at[0, n], S_QD, R_Q0 + n, x=i ^ 1).start()
        rc(qp.at[n, i ^ 1], qr.at[1, n], S_QD, R_Q1, x=i ^ 1).start()

    def gu_part(s, q):
        cols = pl.ds(pl.multiple_of(q * 256, 256), 256)
        hv = h_ref[...]
        return dot(hv, wg_v[s, :, cols]), dot(hv, wu_v[s, :, cols])

    gu_loaded(0)

    def slot0(q, _):
        g, u = gu_part(0, q)
        gs0[q, 0] = g
        gs0[q, 1] = u
        rc(gs0.at[q], r1.at[q], S_G0, R_G0 + q, x=i ^ 1).start()
        return 0

    lax.fori_loop(0, 2, slot0, 0)
    for n in range(3):
        arrived(qr.at[0, n], R_Q0 + n)
        qys[n] = qp[n, i ^ 2] + qr[0, n]
        rc(qys.at[n], qy.at[n], S_QY, R_QY, x=i ^ 2).start()
    lax.fori_loop(2, 4, slot0, 0)
    gu_loaded(1)

    def slot1(q, _):
        g, u = gu_part(1, q)
        arrived(r1.at[q], R_G0 + q)
        ys[q, 0] = g + r1[q, 0]
        ys[q, 1] = u + r1[q, 1]
        rc(ys.at[q], yr.at[q], S_GY, R_GY + q, x=i ^ 2).start()
        return 0

    lax.fori_loop(0, 4, slot1, 0)
    gu_loaded(2)

    def slot2(q, _):
        g, u = gu_part(2, q)
        gs2[q, 0] = g
        gs2[q, 1] = u
        rc(gs2.at[q], r3.at[q], S_G2, R_G2, x=i ^ 1).start()
        return 0

    lax.fori_loop(0, 4, slot2, 0)

    arrived(qr.at[1], R_Q1)
    arrived(qy, R_QY)
    for n in range(3):
        fin = ((qp[n, i] + qr[1, n]) + qy[n]).astype(BF16)
        for b in range(4):
            zs[b, :, n * 384:(n + 1) * 384] = fin[b * 4:(b + 1) * 4, :]
    start([rc(zs.at[j ^ d], zr.at[j], S_QZ, R_QZ, yz=j ^ d) for d in away])
    zr.at[j][...] = zs[j]
    gu_loaded(3)

    def slot3(q, _):
        g, u = gu_part(3, q)
        p3[q, 0] = g
        p3[q, 1] = u
        return 0

    lax.fori_loop(0, 4, slot3, 0)
    arrived(zr.at[0:3], R_QZ)

    cos_t = cs[0]
    sin_t = cs[1]

    def half(k):
        return zr[k // 9, :, (k % 9) * 128:(k % 9 + 1) * 128].astype(F32)

    def rope(k):
        u1, u2 = half(k), half(k + 1)
        return ((u1 * cos_t - u2 * sin_t).astype(BF16).astype(F32), (u2 * cos_t + u1 * sin_t).astype(BF16).astype(F32))

    for hd in range(16):
        t1, t2 = rope(2 * hd)
        qa[hd * 8:hd * 8 + 4, :] = t1
        qb[hd * 8:hd * 8 + 4, :] = t2
    t1, t2 = rope(32)
    kn[0:4, 0:128] = t1
    kn[0:4, 128:256] = t2
    vn[0:4, 0:128] = half(34)
    vn[0:4, 128:256] = half(35)
    later[0].wait()
    later[1].wait()

    def request(r):
        q_r = jnp.concatenate([qa[pl.ds(r, 16, stride=8), :], qb[pl.ds(r, 16, stride=8), :]], axis=1)
        k_new = kn[r:r + 1, :]
        v_new = vn[r:r + 1, :]
        pos_r = len_ref[r]
        s_new = jnp.sum(q_r * k_new, axis=1, keepdims=True) * 0.0625
        qb16 = q_r.astype(BF16)
        for t in range(4):
            sc = lax.dot_general(qb16, ko[r, t * 1024:(t + 1) * 1024, :], (((1,), (1,)), ((), ())),
                                 preferred_element_type=F32) * 0.0625
            pos = t * 1024 + lax.broadcasted_iota(jnp.int32, (16, 1024), 1)
            s_ref[r, :, t * 1024:(t + 1) * 1024] = jnp.where(pos < pos_r, sc, -1e30)
        sc = s_ref[r]
        top = jnp.maximum(jnp.max(sc, axis=1, keepdims=True), s_new)
        e = jnp.exp(sc - top)
        e_new = jnp.exp(s_new - top)
        inv = 1.0 / (jnp.sum(e, axis=1, keepdims=True) + e_new)
        o = (e_new * inv).astype(BF16).astype(F32) * v_new
        o = o + dot((e * inv).astype(BF16), vo[r])
        o = o.astype(BF16).astype(F32)
        osa[r * 16:(r + 1) * 16, :] = o[:, 0:128]
        osb[r * 16:(r + 1) * 16, :] = o[:, 128:256]

    for r in range(4):
        request(r)

    for b in range(4):
        for hh in range(4):
            hd = b * 4 + hh
            oz[b, hh, :, 0:128] = osa[pl.ds(hd, 4, stride=16), :].astype(BF16)
            oz[b, hh, :, 128:256] = osb[pl.ds(hd, 4, stride=16), :].astype(BF16)
    start([rc(oz.at[j ^ d], orr.at[j], S_OZ, R_OZ, yz=j ^ d) for d in away])
    orr.at[j][...] = oz[j]

    def activation(q):
        arrived(yr.at[q], R_GY + q)
        g = ((p3[q, 0] + r3[q, 0]) + yr[q, 0]).astype(BF16).astype(F32)
        u = ((p3[q, 1] + r3[q, 1]) + yr[q, 1]).astype(BF16).astype(F32)
        k = i * 4 + q
        a_all.at[k][...] = (g * jax.nn.sigmoid(g) * u).astype(BF16)
        rc(a_all.at[k], a_all.at[k], S_AY, R_AY + q, x=i ^ 2).start()
        rc(a_all.at[k], a_all.at[k], S_AD, R_AD, x=i ^ 1).start()

    arrived(r3, R_G2)
    activation(0)
    activation(1)
    activation(2)
    activation(3)

    later[2].wait()
    z_buf[...] = jnp.zeros_like(z_buf)

    def z_add(k):
        av = a_all[k]
        rows = pl.ds(pl.multiple_of(k * 256, 256), 256)
        for n in range(4):
            z_buf[n] += dot(av, wmo_v[rows, n * 256:(n + 1) * 256])

    def z_own(q, _):
        z_add(i * 4 + q)
        return 0

    def z_partner(q, _):
        z_add((i ^ 1) * 4 + q)
        return 0

    def z_far(q, _):
        k = (i ^ 2) * 4 + q
        arrived(a_all.at[k], R_AY + q)
        rc(a_all.at[k], a_all.at[k], S_AF, R_AF + q // 3, x=i ^ 1).start()
        z_add(k)
        return 0

    def z_fwd(q, _):
        z_add((i ^ 3) * 4 + q)
        return 0

    lax.fori_loop(0, 4, z_own, 0)
    arrived(orr.at[0:3], R_OZ)
    for hh in range(4):
        o_all.at[i][hh] = jnp.concatenate([orr[b, hh].astype(F32) for b in range(4)], axis=0).astype(BF16)
    start([rc(o_all.at[i], o_all.at[i], S_OX, R_OX, x=i ^ d) for d in (2, 3, 1)])

    arrived(a_all.at[0:4], R_AD)
    lax.fori_loop(0, 4, z_partner, 0)
    lax.fori_loop(0, 4, z_far, 0)
    arrived(a_all.at[0:3], R_AF)
    lax.fori_loop(0, 3, z_fwd, 0)

    arrived(o_all.at[0:3], R_OX)
    later[3].wait()
    ov = [jnp.concatenate([o_all[b, hh] for b in range(4)], axis=0) for hh in range(4)]
    ov = jnp.concatenate(ov, axis=1)
    for n in range(4):
        z_buf[n] += dot(ov, wao_v[:, n * 256:(n + 1) * 256])
    arrived(a_all.at[0], R_AF + 1)
    k = (i ^ 3) * 4 + 3
    rows = pl.ds(pl.multiple_of(k * 256, 256), 256)
    for d in (3, 2, 1, 0):
        cols = pl.ds(pl.multiple_of((j ^ d) * 256, 256), 256)
        z_buf.at[j ^ d][...] += dot(a_all[k], wmo_v[rows, cols])
        if d:
            rc(z_buf.at[j ^ d], z_rec.at[d - 1], S_Z, R_Z, yz=j ^ d).start()

    def insert(r, _):
        k_new = kn[pl.ds(r, 1), :].astype(BF16)
        v_new = vn[pl.ds(r, 1), :].astype(BF16)
        pos_r = len_ref[r]

        def chunk(t, _):
            rows = pl.ds(pl.multiple_of(t * 256, 256), 256)
            pos = t * 256 + lax.broadcasted_iota(jnp.int32, (256, 256), 0)
            ko[r, rows, :] = jnp.where(pos == pos_r, k_new, ko[r, rows, :])
            vo[r, rows, :] = jnp.where(pos == pos_r, v_new, vo[r, rows, :])
            return 0

        return lax.fori_loop(0, 16, chunk, 0)

    lax.fori_loop(0, 4, insert, 0)

    for ref, s in ((st.at[0:3], S_LS), (xg.at[0:3], S_LX), (gs.at[0:3], S_LG), (sz.at[0:3], S_LZ), (qr, S_QD),
                   (qys, S_QY), (zs.at[0:3], S_QZ), (gs0, S_G0), (ys, S_GY), (gs2, S_G2), (a_all.at[0:4], S_AD),
                   (a_all.at[0:4], S_AY), (a_all.at[0:4], S_AF), (oz.at[0:3], S_OZ), (o_all.at[0:3], S_OX)):
        sent(ref, s)
    arrived(z_rec, R_Z)
    z = (z_buf[j] + z_rec[0]) + (z_rec[1] + z_rec[2])
    y_ref[...] = (xg[j].astype(F32) + z).astype(BF16)
    sent(z_rec, S_Z)


def write_kernel(y_in, ki, vi, y_out, ko, vo, sem):
    copies = [pltpu.make_async_copy(ki, ko, sem.at[0]), pltpu.make_async_copy(vi, vo, sem.at[1]),
              pltpu.make_async_copy(y_in, y_out, sem.at[2])]
    for c in copies:
        c.start()
    for c in copies:
        c.wait()


def solution(mesh):
    both_axes = ("x", "yz")
    row_spec = P("dp", both_axes)
    in_w_spec = P("x", "yz")
    out_w_spec = P("yz", "x")
    cache_spec = P(("dp", "x", "yz"), None, None)
    len_spec = P(("dp", "x", "yz"))

    def local_layer(x_loc, gain_loc, wqkv, wg, wu, wao, wmo, kc, vc, len_loc):
        half_dim = kc.shape[2] // 2
        inv_freq = np.float32(10000.0) ** (-np.arange(half_dim, dtype=np.float32) / np.float32(half_dim))
        vm = pl.BlockSpec(memory_space=pltpu.VMEM)
        hbm = pl.BlockSpec(memory_space=pl.ANY)
        gu = pltpu.VMEM((4, 2, 64, 256), F32)
        y, ko, vo = pl.pallas_call(
            layer_kernel, name="layer",
            out_shape=(pltpu.VMEM(x_loc.shape, BF16), pltpu.VMEM(kc.shape, BF16), pltpu.VMEM(vc.shape, BF16)),
            in_specs=[hbm] * 11,
            out_specs=(vm, vm, vm),
            scratch_shapes=[
                pltpu.VMEM((256,), BF16), pltpu.VMEM((1, 128), F32), pltpu.SMEM((4,), jnp.int32),
                pltpu.VMEM((1024, 1152), BF16), pltpu.VMEM((4, 1024, 1024), BF16), pltpu.VMEM((4, 1024, 1024), BF16),
                pltpu.VMEM((1024, 1024), BF16), pltpu.VMEM((4096, 1024), BF16),
                pltpu.VMEM((4, 64, 256), BF16), pltpu.VMEM((4, 1, 256), F32),
                pltpu.VMEM((4, 1, 128), F32), pltpu.VMEM((4, 1, 128), F32), pltpu.VMEM((2, 4, 128), F32),
                pltpu.VMEM((64, 1024), BF16),
                pltpu.VMEM((3, 4, 16, 384), F32), pltpu.VMEM((2, 3, 16, 384), F32), pltpu.VMEM((3, 16, 384), F32),
                pltpu.VMEM((3, 16, 384), F32), pltpu.VMEM((4, 4, 1152), BF16), pltpu.VMEM((4, 4, 1152), BF16),
                pltpu.VMEM((128, 128), F32), pltpu.VMEM((128, 128), F32), pltpu.VMEM((8, 256), F32),
                pltpu.VMEM((8, 256), F32), pltpu.VMEM((4, 16, 4096), F32), pltpu.VMEM((64, 128), F32),
                pltpu.VMEM((64, 128), F32),
                gu, gu, gu, gu, gu, gu, gu,
                pltpu.VMEM((16, 64, 256), BF16), pltpu.VMEM((4, 4, 4, 256), BF16), pltpu.VMEM((4, 4, 4, 256), BF16),
                pltpu.VMEM((4, 4, 16, 256), BF16), pltpu.VMEM((4, 64, 256), F32), pltpu.VMEM((3, 64, 256), F32),
                pltpu.SemaphoreType.DMA((N_LOAD,)), pltpu.SemaphoreType.DMA((N_SEND,)), pltpu.SemaphoreType.DMA((N_RECV,)),
            ],
            compiler_params=pltpu.CompilerParams(collective_id=0, has_side_effects=True,
                                                 vmem_limit_bytes=46 * 1024 * 1024),
        )(x_loc, gain_loc, inv_freq.reshape(1, -1), len_loc, wqkv, wg, wu, wao, wmo, kc, vc)
        return pl.pallas_call(
            write_kernel, name="write",
            out_shape=tuple(jax.ShapeDtypeStruct(a.shape, BF16) for a in (x_loc, kc, vc)),
            in_specs=[vm] * 3,
            out_specs=[hbm] * 3,
            scratch_shapes=[pltpu.SemaphoreType.DMA((3,))],
            compiler_params=pltpu.CompilerParams(vmem_limit_bytes=8 * 1024 * 1024),
        )(y, ko, vo)

    in_specs = (row_spec, P(both_axes), in_w_spec, in_w_spec, in_w_spec, out_w_spec, out_w_spec, cache_spec, cache_spec, len_spec)
    out_specs = (row_spec, cache_spec, cache_spec)
    return jax.shard_map(local_layer, mesh=mesh, in_specs=in_specs, out_specs=out_specs, check_vma=False)
```

```python
import jax
import numpy as np
import jax.numpy as jnp
from jax import lax
from jax.sharding import PartitionSpec as P
from jax.experimental import pallas as pl
from jax.experimental.pallas import tpu as pltpu

MESH = pl.DeviceIdType.MESH
F32 = jnp.float32
BF16 = jnp.bfloat16

ROWS, BLK, QROWS, DEV, THIRD, FF = 64, 256, 16, 4, 384, 1024
HALF = BLK // 2
CORES = range(DEV)
AWAY = (3, 2, 1)


def slots(text):
    out, at = {}, 0
    for word in text.split():
        name, _, n = word.partition("*")
        out[name] = at
        at += int(n or 1)
    return out, at


SEND, N_SEND = slots("lx lg ls" " qd qy qz g0" " gy g2 ad ay" " af oz ox z")
RECV, N_RECV = slots("lx lg ls" " q0*3 q1 qy qz" " g0*4 gy*4 g2 ad*2" " ay*4 af*2 oz ox" " z")
LOAD, N_LOAD = slots("x qkv gu*4 k" " v mo ao small*3")


def vmem(dtype, *shape):
    return pltpu.VMEM(shape, dtype)


def dot(a, b):
    return jnp.dot(a, b, preferred_element_type=F32)


def layer_kernel(x_hbm, g_hbm, freq_hbm, len_hbm, wqkv, wg, wu, wao, wmo, kc, vc,
                 y_ref, ko, vo,
                 g_v, freq_v, len_ref, wqkv_v, wg_v, wu_v, wao_v, wmo_v,
                 xg, gs, st, cs, h_ref, qp, qr, qys, qy, zs, zr, qa, qb, kn, vn, s_ref, osa, osb,
                 gs0, r1, ys, yr, gs2, r3, p3, a_all, oz, orr, o_all, z_buf, z_rec,
                 lsem, ssem, rsem):
    i = lax.axis_index("x")
    j = lax.axis_index("yz")
    d_model = 16 * x_hbm.shape[1]
    inner = (j + 1) // 2 % 2
    far = (3 - inner, 2 + inner, 1)

    def rc(src, dst, s, r, **dev):
        return pltpu.make_async_remote_copy(src_ref=src, dst_ref=dst, send_sem=ssem.at[s], recv_sem=rsem.at[r],
                                            device_id=dev, device_id_type=MESH)

    def start(copies):
        for c in copies:
            c.start()

    def arrived(ref, r):
        rc(ref, ref, 0, r, x=i ^ 1).wait_recv()

    def sent(ref, s):
        rc(ref, ref, s, 0, x=i ^ 1).wait_send()

    barrier = pltpu.get_barrier_semaphore()
    group = [(n % DEV, n // DEV) for n in range(1, QROWS)]
    for dx, dz in group:
        pl.semaphore_signal(barrier, inc=1, device_id={"x": i ^ dx, "yz": j ^ dz}, device_id_type=MESH)
    small = [pltpu.make_async_copy(x_hbm, xg.at[j], lsem.at[LOAD["x"]]),
             pltpu.make_async_copy(g_hbm, g_v, lsem.at[LOAD["small"]]),
             pltpu.make_async_copy(freq_hbm, freq_v, lsem.at[LOAD["small"] + 1]),
             pltpu.make_async_copy(len_hbm, len_ref, lsem.at[LOAD["small"] + 2])]
    start(small)
    qkv_load = pltpu.make_async_copy(wqkv, wqkv_v, lsem.at[LOAD["qkv"]])
    qkv_load.start()
    for s in CORES:
        cols = pl.ds(pl.multiple_of((i ^ (3 - s)) * 1024, 1024), 1024)
        pltpu.make_async_copy(wg.at[:, cols], wg_v.at[s], lsem.at[LOAD["gu"] + s]).start()
        pltpu.make_async_copy(wu.at[:, cols], wu_v.at[s], lsem.at[LOAD["gu"] + s]).start()

    def gu_loaded(s):
        pltpu.make_async_copy(wg_v.at[0:2], wg_v.at[0:2], lsem.at[LOAD["gu"] + s]).wait()

    later = [pltpu.make_async_copy(kc, ko, lsem.at[LOAD["k"]]), pltpu.make_async_copy(vc, vo, lsem.at[LOAD["v"]]),
             pltpu.make_async_copy(wmo, wmo_v, lsem.at[LOAD["mo"]]), pltpu.make_async_copy(wao, wao_v, lsem.at[LOAD["ao"]])]

    for c in small:
        c.wait()
    gs.at[j][...] = g_v[...].reshape(1, 256).astype(F32)
    xf = xg[j].astype(F32)
    s1 = jnp.sum(xf, axis=1, keepdims=True)
    s2 = jnp.sum(xf * xf, axis=1, keepdims=True)
    stat = jnp.broadcast_to(jnp.concatenate([s1, s2], axis=0), (128, 128))
    me = j * DEV + i
    st.at[me][...] = stat.T[0:1, :]
    pl.semaphore_wait(barrier, QROWS - 1)

    start([rc(st.at[me], st.at[me], SEND["ls"], RECV["ls"], x=i ^ dx, yz=j ^ dz) for dx, dz in reversed(group)])
    start([rc(xg.at[j], xg.at[j], SEND["lx"], RECV["lx"], yz=j ^ d) for d in far])
    start([rc(gs.at[j], gs.at[j], SEND["lg"], RECV["lg"], yz=j ^ d) for d in far])
    start(later)
    row = lax.broadcasted_iota(jnp.int32, (4, 128), 0)
    pos = jnp.zeros((4, 128), F32)
    for r in CORES:
        pos = jnp.where(row == r, len_ref[r].astype(F32), pos)
    angle = pos * freq_v[...]
    cs[0] = jnp.cos(angle)
    cs[1] = jnp.sin(angle)
    arrived(st.at[:QROWS - 1], RECV["ls"])
    arrived(gs.at[:3], RECV["lg"])
    arrived(xg.at[:3], RECV["lx"])
    tot = st[0]
    for n in range(1, QROWS):
        tot = tot + st[n]
    tot = jnp.broadcast_to(tot, (128, 128)).T
    mean = tot[0:64, 0:1] / d_model
    var = tot[64:128, 0:1] / d_model - mean * mean
    rstd = lax.rsqrt(var + 1e-6)
    for jj in CORES:
        xb = xg[jj].astype(F32)
        h_ref[:, jj * 256:(jj + 1) * 256] = ((xb - mean) * rstd * gs[jj]).astype(BF16)

    qkv_load.wait()
    for n in range(3):
        part = dot(h_ref[...], wqkv_v[:, n * 384:(n + 1) * 384])
        for b in CORES:
            qp[n, b] = part[b * 16:(b + 1) * 16, :]
        if n:
            rc(qp.at[n, i ^ 3], qr.at[0, n], SEND["qd"], RECV["q0"] + n, x=i ^ 1).start()
        else:
            rc(qp.at[n, i ^ 2], qy.at[n], SEND["qy"], RECV["qy"], x=i ^ 2).start()
            rc(qp.at[n, i ^ 3], qr.at[0, n], SEND["qd"], RECV["q0"], x=i ^ 3).start()
        rc(qp.at[n, i ^ 1], qr.at[1, n], SEND["qd"], RECV["q1"], x=i ^ 1).start()

    def gu_part(s, q):
        cols = pl.ds(pl.multiple_of(q * 256, 256), 256)
        hv = h_ref[...]
        return dot(hv, wg_v[s, :, cols]), dot(hv, wu_v[s, :, cols])

    gu_loaded(0)

    def slot0(q, _):
        g, u = gu_part(0, q)
        gs0[q, 0] = g
        gs0[q, 1] = u
        rc(gs0.at[q], r1.at[q], SEND["g0"], RECV["g0"] + q, x=i ^ 1).start()
        return 0

    lax.fori_loop(0, 2, slot0, 0)
    for n in range(1, 3):
        arrived(qr.at[0, n], RECV["q0"] + n)
        qys[n] = qp[n, i ^ 2] + qr[0, n]
        rc(qys.at[n], qy.at[n], SEND["qy"], RECV["qy"], x=i ^ 2).start()
    def slot1(q, _):
        g, u = gu_part(1, q)
        arrived(r1.at[q], RECV["g0"] + q)
        ys[q, 0] = g + r1[q, 0]
        ys[q, 1] = u + r1[q, 1]
        rc(ys.at[q], yr.at[q], SEND["gy"], RECV["gy"] + q, x=i ^ 2).start()
        return 0

    gu_loaded(1)

    def slot01(q, _):
        slot1(q, 0)
        return slot0(q + 2, 0)

    lax.fori_loop(0, 2, slot01, 0)
    lax.fori_loop(2, 4, slot1, 0)
    gu_loaded(2)

    def slot2(q, _):
        g, u = gu_part(2, q)
        gs2[q, 0] = g
        gs2[q, 1] = u
        rc(gs2.at[q], r3.at[q], SEND["g2"], RECV["g2"], x=i ^ 1).start()
        return 0

    lax.fori_loop(0, 4, slot2, 0)

    arrived(qr.at[1], RECV["q1"])
    arrived(qy, RECV["qy"])
    arrived(qr.at[0, 0], RECV["q0"])
    for n in range(3):
        other = qy[n] if n else qy[n] + qr[0, n]
        fin = ((qp[n, i] + qr[1, n]) + other).astype(BF16)
        for b in CORES:
            zs[b, :, n * 384:(n + 1) * 384] = fin[b * 4:(b + 1) * 4, :]
    start([rc(zs.at[j ^ d], zr.at[j], SEND["qz"], RECV["qz"], yz=j ^ d) for d in far])
    zr.at[j][...] = zs[j]
    gu_loaded(3)

    def slot3(q, _):
        g, u = gu_part(3, q)
        p3[q, 0] = g
        p3[q, 1] = u
        return 0

    lax.fori_loop(0, 4, slot3, 0)
    arrived(zr.at[:3], RECV["qz"])

    cos_t = cs[0]
    sin_t = cs[1]

    def half(k):
        return zr[k // 9, :, (k % 9) * 128:(k % 9 + 1) * 128].astype(F32)

    def rope(k):
        u1, u2 = half(k), half(k + 1)
        return ((u1 * cos_t - u2 * sin_t).astype(BF16).astype(F32), (u2 * cos_t + u1 * sin_t).astype(BF16).astype(F32))

    for hd in range(16):
        t1, t2 = rope(2 * hd)
        qa[hd * 8:hd * 8 + 4, :] = t1
        qb[hd * 8:hd * 8 + 4, :] = t2
    t1, t2 = rope(32)
    kn[0:4, 0:128] = t1
    kn[0:4, 128:256] = t2
    vn[0:4, 0:128] = half(34)
    vn[0:4, 128:256] = half(35)
    later[0].wait()
    later[1].wait()

    def scores(r):
        q_r = jnp.concatenate([qa[pl.ds(r, 16, stride=8), :], qb[pl.ds(r, 16, stride=8), :]], axis=1)
        pos_r = len_ref[r]
        qb16 = q_r.astype(BF16)
        for t in CORES:
            sc = lax.dot_general(qb16, ko[r, t * 1024:(t + 1) * 1024, :], (((1,), (1,)), ((), ())),
                                 preferred_element_type=F32) * 0.0625
            pos = t * 1024 + lax.broadcasted_iota(jnp.int32, (16, 1024), 1)
            s_ref[r, :, t * 1024:(t + 1) * 1024] = jnp.where(pos < pos_r, sc, -1e30)
        return jnp.sum(q_r * kn[r:r + 1, :], axis=1, keepdims=True) * 0.0625

    def values(r, s_new):
        sc = s_ref[r]
        top = jnp.maximum(jnp.max(sc, axis=1, keepdims=True), s_new)
        e = jnp.exp(sc - top)
        e_new = jnp.exp(s_new - top)
        inv = 1.0 / (jnp.sum(e, axis=1, keepdims=True) + e_new)
        o = (e_new * inv).astype(BF16).astype(F32) * vn[r:r + 1, :]
        o = o + dot((e * inv).astype(BF16), vo[r])
        o = o.astype(BF16).astype(F32)
        osa[r * 16:(r + 1) * 16, :] = o[:, 0:128]
        osb[r * 16:(r + 1) * 16, :] = o[:, 128:256]

    s_new = [scores(0)]
    for r in range(1, DEV):
        s_new.append(scores(r))
        values(r - 1, s_new[r - 1])
    values(r, s_new[r])

    for b in CORES:
        for hh in CORES:
            hd = b * 4 + hh
            oz[b, hh, :, 0:128] = osa[pl.ds(hd, 4, stride=16), :].astype(BF16)
            oz[b, hh, :, 128:256] = osb[pl.ds(hd, 4, stride=16), :].astype(BF16)
    start([rc(oz.at[j ^ d], orr.at[j], SEND["oz"], RECV["oz"], yz=j ^ d) for d in far])
    orr.at[j][...] = oz[j]

    def activation(q):
        arrived(yr.at[q], RECV["gy"] + q)
        g = ((p3[q, 0] + r3[q, 0]) + yr[q, 0]).astype(BF16).astype(F32)
        u = ((p3[q, 1] + r3[q, 1]) + yr[q, 1]).astype(BF16).astype(F32)
        k = i * 4 + q
        a_all.at[k][...] = (g * jax.nn.sigmoid(g) * u).astype(BF16)
        rc(a_all.at[k], a_all.at[k], SEND["ay"], RECV["ay"] + q, x=i ^ 2).start()
        rc(a_all.at[k], a_all.at[k], SEND["ad"], RECV["ad"] + q // 3, x=i ^ 1).start()

    arrived(r3, RECV["g2"])
    for q in range(3):
        activation(q)

    later[2].wait()
    z_buf[...] = jnp.zeros_like(z_buf)

    def z_add(k):
        av = a_all[k]
        rows = pl.ds(pl.multiple_of(k * 256, 256), 256)
        for n in CORES:
            z_buf[n] += dot(av, wmo_v[rows, n * 256:(n + 1) * 256])

    def z_own(q, _):
        z_add(i * 4 + q)
        return 0

    def z_partner(q, _):
        z_add((i ^ 1) * 4 + q)
        return 0

    def z_far(q, _):
        k = (i ^ 2) * 4 + q
        arrived(a_all.at[k], RECV["ay"] + q)
        rc(a_all.at[k], a_all.at[k], SEND["af"], RECV["af"] + q // 3, x=i ^ 1).start()
        z_add(k)
        return 0

    def z_fwd(q, _):
        z_add((i ^ 3) * 4 + q)
        return 0

    lax.fori_loop(0, 3, z_own, 0)
    arrived(a_all.at[:3], RECV["ad"])
    lax.fori_loop(0, 3, z_partner, 0)
    activation(3)
    arrived(orr.at[:3], RECV["oz"])
    for hh in CORES:
        o_all.at[i][hh] = jnp.concatenate([orr[b, hh].astype(F32) for b in CORES], axis=0).astype(BF16)
    start([rc(o_all.at[i], o_all.at[i], SEND["ox"], RECV["ox"], x=i ^ d) for d in (2, 3, 1)])
    lax.fori_loop(3, 4, z_own, 0)
    lax.fori_loop(0, 3, z_far, 0)
    arrived(a_all.at[0], RECV["ad"] + 1)
    lax.fori_loop(3, 4, z_partner, 0)
    lax.fori_loop(3, 4, z_far, 0)
    arrived(a_all.at[:3], RECV["af"])
    lax.fori_loop(0, 3, z_fwd, 0)

    arrived(o_all.at[:3], RECV["ox"])
    later[3].wait()
    ov = [jnp.concatenate([o_all[b, hh] for b in CORES], axis=0) for hh in CORES]
    ov = jnp.concatenate(ov, axis=1)
    for n in CORES:
        z_buf[n] += dot(ov, wao_v[:, n * 256:(n + 1) * 256])
    arrived(a_all.at[0], RECV["af"] + 1)
    k = (i ^ 3) * 4 + 3
    rows = pl.ds(pl.multiple_of(k * 256, 256), 256)
    for d in far + (0,):
        cols = pl.ds(pl.multiple_of((j ^ d) * 256, 256), 256)
        z_buf.at[j ^ d][...] += dot(a_all[k], wmo_v[rows, cols])
        if not isinstance(d, int) or d:
            rc(z_buf.at[j ^ d], z_rec.at[d - 1], SEND["z"], RECV["z"], yz=j ^ d).start()

    def insert(r, _):
        k_new = kn[pl.ds(r, 1), :].astype(BF16)
        v_new = vn[pl.ds(r, 1), :].astype(BF16)
        pos_r = len_ref[r]

        def chunk(t, _):
            rows = pl.ds(pl.multiple_of(t * 256, 256), 256)
            pos = t * 256 + lax.broadcasted_iota(jnp.int32, (256, 256), 0)
            ko[r, rows, :] = jnp.where(pos == pos_r, k_new, ko[r, rows, :])
            vo[r, rows, :] = jnp.where(pos == pos_r, v_new, vo[r, rows, :])
            return 0

        return lax.fori_loop(0, 16, chunk, 0)

    lax.fori_loop(0, 4, insert, 0)

    for ref, s in ((st.at[:QROWS - 1], SEND["ls"]), (xg.at[:3], SEND["lx"]), (gs.at[:3], SEND["lg"]), (qr, SEND["qd"]),
                   (qys, SEND["qy"]), (zs.at[:3], SEND["qz"]), (gs0, SEND["g0"]), (ys, SEND["gy"]), (gs2, SEND["g2"]), (a_all.at[0:4], SEND["ad"]),
                   (a_all.at[0:4], SEND["ay"]), (a_all.at[0:4], SEND["af"]), (oz.at[:3], SEND["oz"]), (o_all.at[:3], SEND["ox"])):
        sent(ref, s)
    arrived(z_rec, RECV["z"])
    z = (z_buf[j] + z_rec[0]) + (z_rec[1] + z_rec[2])
    y_ref[...] = (xg[j].astype(F32) + z).astype(BF16)
    sent(z_rec, SEND["z"])


def write_kernel(y_in, ki, vi, y_out, ko, vo, sem):
    copies = [pltpu.make_async_copy(ki, ko, sem.at[0]), pltpu.make_async_copy(vi, vo, sem.at[1]),
              pltpu.make_async_copy(y_in, y_out, sem.at[2])]
    for c in copies:
        c.start()
    for c in copies:
        c.wait()


def solution(mesh):
    both_axes = ("x", "yz")
    row_spec = P("dp", both_axes)
    in_w_spec = P("x", "yz")
    out_w_spec = P("yz", "x")
    cache_spec = P(("dp", "x", "yz"), None, None)
    len_spec = P(("dp", "x", "yz"))

    def local_layer(x_loc, gain_loc, wqkv, wg, wu, wao, wmo, kc, vc, len_loc):
        half_dim = kc.shape[2] // 2
        inv_freq = np.float32(10000.0) ** (-np.arange(half_dim, dtype=np.float32) / np.float32(half_dim))
        vm = pl.BlockSpec(memory_space=pltpu.VMEM)
        hbm = pl.BlockSpec(memory_space=pl.ANY)
        y, ko, vo = pl.pallas_call(
            layer_kernel, name="layer",
            out_shape=(pltpu.VMEM(x_loc.shape, BF16), pltpu.VMEM(kc.shape, BF16), pltpu.VMEM(vc.shape, BF16)),
            in_specs=[hbm] * 11,
            out_specs=(vm, vm, vm),
            scratch_shapes=[
                vmem(BF16, BLK), vmem(F32, 1, HALF), pltpu.SMEM((DEV,), jnp.int32),
                vmem(BF16, FF, wqkv.shape[1]), vmem(BF16, DEV, FF, FF), vmem(BF16, DEV, FF, FF),
                vmem(BF16, *wao.shape), vmem(BF16, *wmo.shape),
                vmem(BF16, DEV, ROWS, BLK), vmem(F32, DEV, 1, BLK), vmem(F32, QROWS, 1, HALF),
                vmem(F32, 2, DEV, HALF), vmem(BF16, ROWS, FF),
                vmem(F32, 3, DEV, QROWS, THIRD), vmem(F32, 2, 3, QROWS, THIRD), vmem(F32, 3, QROWS, THIRD),
                vmem(F32, 3, QROWS, THIRD), vmem(BF16, DEV, DEV, 3 * THIRD), vmem(BF16, DEV, DEV, 3 * THIRD),
                vmem(F32, HALF, HALF), vmem(F32, HALF, HALF), vmem(F32, 8, BLK), vmem(F32, 8, BLK),
                vmem(F32, DEV, QROWS, kc.shape[1]), vmem(F32, ROWS, HALF), vmem(F32, ROWS, HALF)]
            + [vmem(F32, DEV, 2, ROWS, BLK)] * 7
            + [vmem(BF16, QROWS, ROWS, BLK), vmem(BF16, DEV, DEV, DEV, BLK), vmem(BF16, DEV, DEV, DEV, BLK),
               vmem(BF16, DEV, DEV, QROWS, BLK), vmem(F32, DEV, ROWS, BLK), vmem(F32, 3, ROWS, BLK)]
            + [pltpu.SemaphoreType.DMA((n,)) for n in (N_LOAD, N_SEND, N_RECV)],
            compiler_params=pltpu.CompilerParams(collective_id=0, has_side_effects=True,
                                                 vmem_limit_bytes=46 * 1024 * 1024),
        )(x_loc, gain_loc, inv_freq.reshape(1, -1), len_loc, wqkv, wg, wu, wao, wmo, kc, vc)
        return pl.pallas_call(
            write_kernel, name="write",
            out_shape=tuple(jax.ShapeDtypeStruct(a.shape, BF16) for a in (x_loc, kc, vc)),
            in_specs=[vm] * 3,
            out_specs=[hbm] * 3,
            scratch_shapes=[pltpu.SemaphoreType.DMA((3,))],
            compiler_params=pltpu.CompilerParams(vmem_limit_bytes=8 * 1024 * 1024),
        )(y, ko, vo)

    in_specs = (row_spec, P(both_axes), in_w_spec, in_w_spec, in_w_spec, out_w_spec, out_w_spec, cache_spec, cache_spec, len_spec)
    out_specs = (row_spec, cache_spec, cache_spec)
    return jax.shard_map(local_layer, mesh=mesh, in_specs=in_specs, out_specs=out_specs, check_vma=False)
```

```python
import jax
import numpy as np
import jax.numpy as jnp
from jax import lax
from jax.sharding import PartitionSpec as P
from jax.experimental import pallas as pl
from jax.experimental.pallas import tpu as pltpu

MESH = pl.DeviceIdType.MESH
F32 = jnp.float32
BF16 = jnp.bfloat16

ROWS, BLK, QROWS, DEV, THIRD, FF = 64, 256, 16, 4, 384, 1024
HALF = BLK // 2
CORES = range(DEV)
AWAY = (3, 2, 1)


def slots(*words):
    out, at = {}, 0
    for word in " ".join(words).split():
        name, _, n = word.partition("*")
        out[name] = at
        at += int(n or 1)
    return out, at


SEND, N_SEND = slots("lx lg ls", "qd qy qz g0", "gy g2 ad ay", "af oz ox z")
RECV, N_RECV = slots("lx lg ls", "q0*3 q1 qy qz", "g0*4 gy*4 g2 ad*2", "ay*4 af*2 oz ox", "z")
LOAD, N_LOAD = slots("x qkv gu*4 k", "v mo ao small*3")


def vmem(dtype, *shape):
    return pltpu.VMEM(shape, dtype)


def dot(a, b):
    return jnp.dot(a, b, preferred_element_type=F32)


def layer_kernel(x_hbm, g_hbm, freq_hbm, len_hbm, wqkv, wg, wu, wao, wmo, kc, vc,
                 z0, z1, z2, z3, ko, vo,
                 g_v, freq_v, len_ref, wqkv_v, wg_v, wu_v, wao_v, wmo_v,
                 xg, gs, st, cs, h_ref, qp, qr, qys, qy, zs, zr, qa, qb, kn, vn, s_ref, osa, osb,
                 gs0, r1, ys, yr, gs2, r3, p3, a_all, oz, orr, o_all, z_buf,
                 lsem, ssem, rsem):
    i = lax.axis_index("x")
    j = lax.axis_index("yz")
    d_model = 16 * x_hbm.shape[1]
    inner = (j + 1) // 2 % 2
    far = (3 - inner, 2 + inner, 1)

    def rc(src, dst, s, r, **dev):
        return pltpu.make_async_remote_copy(src_ref=src, dst_ref=dst, send_sem=ssem.at[s], recv_sem=rsem.at[r],
                                            device_id=dev, device_id_type=MESH)

    def start(copies):
        for c in copies:
            c.start()

    def arrived(ref, r):
        rc(ref, ref, 0, r, x=i ^ 1).wait_recv()

    def sent(ref, s):
        rc(ref, ref, s, 0, x=i ^ 1).wait_send()

    barrier = pltpu.get_barrier_semaphore()
    group = [(n % DEV, n // DEV) for n in range(1, QROWS)]
    for dx, dz in group:
        pl.semaphore_signal(barrier, inc=1, device_id={"x": i ^ dx, "yz": j ^ dz}, device_id_type=MESH)
    small = [pltpu.make_async_copy(x_hbm, xg.at[j], lsem.at[LOAD["x"]]),
             pltpu.make_async_copy(g_hbm, g_v, lsem.at[LOAD["small"]]),
             pltpu.make_async_copy(freq_hbm, freq_v, lsem.at[LOAD["small"] + 1]),
             pltpu.make_async_copy(len_hbm, len_ref, lsem.at[LOAD["small"] + 2])]
    start(small)
    qkv_load = pltpu.make_async_copy(wqkv, wqkv_v, lsem.at[LOAD["qkv"]])
    qkv_load.start()
    for s in CORES:
        cols = pl.ds(pl.multiple_of((i ^ (3 - s)) * 1024, 1024), 1024)
        pltpu.make_async_copy(wg.at[:, cols], wg_v.at[s], lsem.at[LOAD["gu"] + s]).start()
        pltpu.make_async_copy(wu.at[:, cols], wu_v.at[s], lsem.at[LOAD["gu"] + s]).start()

    def gu_loaded(s):
        pltpu.make_async_copy(wg_v.at[0:2], wg_v.at[0:2], lsem.at[LOAD["gu"] + s]).wait()

    later = [pltpu.make_async_copy(kc, ko, lsem.at[LOAD["k"]]), pltpu.make_async_copy(vc, vo, lsem.at[LOAD["v"]]),
             pltpu.make_async_copy(wmo, wmo_v, lsem.at[LOAD["mo"]]), pltpu.make_async_copy(wao, wao_v, lsem.at[LOAD["ao"]])]

    for c in small:
        c.wait()
    gs.at[j][...] = g_v[...].reshape(1, 256).astype(F32)
    xf = xg[j].astype(F32)
    s1 = jnp.sum(xf, axis=1, keepdims=True)
    s2 = jnp.sum(xf * xf, axis=1, keepdims=True)
    stat = jnp.broadcast_to(jnp.concatenate([s1, s2], axis=0), (128, 128))
    me = j * DEV + i
    st.at[me][...] = stat.T[0:1, :]
    pl.semaphore_wait(barrier, QROWS - 1)

    start([rc(st.at[me], st.at[me], SEND["ls"], RECV["ls"], x=i ^ dx, yz=j ^ dz) for dx, dz in reversed(group)])
    start([rc(xg.at[j], xg.at[j], SEND["lx"], RECV["lx"], yz=j ^ d) for d in far])
    start([rc(gs.at[j], gs.at[j], SEND["lg"], RECV["lg"], yz=j ^ d) for d in far])
    start(later)
    row = lax.broadcasted_iota(jnp.int32, (4, 128), 0)
    pos = jnp.zeros((4, 128), F32)
    for r in CORES:
        pos = jnp.where(row == r, len_ref[r].astype(F32), pos)
    angle = pos * freq_v[...]
    cs[0] = jnp.cos(angle)
    cs[1] = jnp.sin(angle)
    arrived(st.at[:QROWS - 1], RECV["ls"])
    arrived(gs.at[:3], RECV["lg"])
    arrived(xg.at[:3], RECV["lx"])
    tot = st[0]
    for n in range(1, QROWS):
        tot = tot + st[n]
    tot = jnp.broadcast_to(tot, (128, 128)).T
    mean = tot[0:64, 0:1] / d_model
    var = tot[64:128, 0:1] / d_model - mean * mean
    rstd = lax.rsqrt(var + 1e-6)
    for jj in CORES:
        xb = xg[jj].astype(F32)
        h_ref[:, jj * 256:(jj + 1) * 256] = ((xb - mean) * rstd * gs[jj]).astype(BF16)

    qkv_load.wait()
    for n in range(3):
        part = dot(h_ref[...], wqkv_v[:, n * 384:(n + 1) * 384])
        for b in CORES:
            qp[n, b] = part[b * 16:(b + 1) * 16, :]
        if n:
            rc(qp.at[n, i ^ 3], qr.at[0, n], SEND["qd"], RECV["q0"] + n, x=i ^ 1).start()
        else:
            rc(qp.at[n, i ^ 2], qy.at[n], SEND["qy"], RECV["qy"], x=i ^ 2).start()
            rc(qp.at[n, i ^ 3], qr.at[0, n], SEND["qd"], RECV["q0"], x=i ^ 3).start()
        rc(qp.at[n, i ^ 1], qr.at[1, n], SEND["qd"], RECV["q1"], x=i ^ 1).start()

    def gu_part(s, q):
        cols = pl.ds(pl.multiple_of(q * 256, 256), 256)
        hv = h_ref[...]
        return dot(hv, wg_v[s, :, cols]), dot(hv, wu_v[s, :, cols])

    gu_loaded(0)

    def slot0(q, _):
        g, u = gu_part(0, q)
        gs0[q, 0] = g
        gs0[q, 1] = u
        rc(gs0.at[q], r1.at[q], SEND["g0"], RECV["g0"] + q, x=i ^ 1).start()
        return 0

    lax.fori_loop(0, 2, slot0, 0)
    for n in range(1, 3):
        arrived(qr.at[0, n], RECV["q0"] + n)
        qys[n] = qp[n, i ^ 2] + qr[0, n]
        rc(qys.at[n], qy.at[n], SEND["qy"], RECV["qy"], x=i ^ 2).start()
    def slot1(q, _):
        g, u = gu_part(1, q)
        arrived(r1.at[q], RECV["g0"] + q)
        ys[q, 0] = g + r1[q, 0]
        ys[q, 1] = u + r1[q, 1]
        rc(ys.at[q], yr.at[q], SEND["gy"], RECV["gy"] + q, x=i ^ 2).start()
        return 0

    gu_loaded(1)

    def slot01(q, _):
        slot1(q, 0)
        return slot0(q + 2, 0)

    lax.fori_loop(0, 2, slot01, 0)
    lax.fori_loop(2, 4, slot1, 0)
    arrived(qr.at[1], RECV["q1"])
    arrived(qy, RECV["qy"])
    arrived(qr.at[0, 0], RECV["q0"])
    for n in range(3):
        other = qy[n] if n else qy[n] + qr[0, n]
        fin = ((qp[n, i] + qr[1, n]) + other).astype(BF16)
        for b in CORES:
            zs[b, :, n * 384:(n + 1) * 384] = fin[b * 4:(b + 1) * 4, :]
    start([rc(zs.at[j ^ d], zr.at[j], SEND["qz"], RECV["qz"], yz=j ^ d) for d in far])
    zr.at[j][...] = zs[j]
    gu_loaded(2)

    def slot2(q, _):
        g, u = gu_part(2, q)
        gs2[q, 0] = g
        gs2[q, 1] = u
        rc(gs2.at[q], r3.at[q], SEND["g2"], RECV["g2"], x=i ^ 1).start()
        return 0

    lax.fori_loop(0, 4, slot2, 0)

    gu_loaded(3)

    def slot3(q, _):
        g, u = gu_part(3, q)
        p3[q, 0] = g
        p3[q, 1] = u
        return 0

    lax.fori_loop(0, 4, slot3, 0)
    arrived(zr.at[:3], RECV["qz"])

    cos_t = cs[0]
    sin_t = cs[1]

    def half(k):
        return zr[k // 9, :, (k % 9) * 128:(k % 9 + 1) * 128].astype(F32)

    def rope(k):
        u1, u2 = half(k), half(k + 1)
        return ((u1 * cos_t - u2 * sin_t).astype(BF16).astype(F32), (u2 * cos_t + u1 * sin_t).astype(BF16).astype(F32))

    for hd in range(16):
        t1, t2 = rope(2 * hd)
        qa[hd * 8:hd * 8 + 4, :] = t1
        qb[hd * 8:hd * 8 + 4, :] = t2
    t1, t2 = rope(32)
    kn[0:4, 0:128] = t1
    kn[0:4, 128:256] = t2
    vn[0:4, 0:128] = half(34)
    vn[0:4, 128:256] = half(35)
    later[0].wait()
    later[1].wait()

    def scores(r):
        q_r = jnp.concatenate([qa[pl.ds(r, 16, stride=8), :], qb[pl.ds(r, 16, stride=8), :]], axis=1)
        pos_r = len_ref[r]
        qb16 = q_r.astype(BF16)
        for t in CORES:
            sc = lax.dot_general(qb16, ko[r, t * 1024:(t + 1) * 1024, :], (((1,), (1,)), ((), ())),
                                 preferred_element_type=F32) * 0.0625
            pos = t * 1024 + lax.broadcasted_iota(jnp.int32, (16, 1024), 1)
            s_ref[r, :, t * 1024:(t + 1) * 1024] = jnp.where(pos < pos_r, sc, -1e30)
        return jnp.sum(q_r * kn[r:r + 1, :], axis=1, keepdims=True) * 0.0625

    def values(r, s_new):
        sc = s_ref[r]
        top = jnp.maximum(jnp.max(sc, axis=1, keepdims=True), s_new)
        e = jnp.exp(sc - top)
        e_new = jnp.exp(s_new - top)
        inv = 1.0 / (jnp.sum(e, axis=1, keepdims=True) + e_new)
        o = (e_new * inv).astype(BF16).astype(F32) * vn[r:r + 1, :]
        o = o + dot((e * inv).astype(BF16), vo[r])
        o = o.astype(BF16).astype(F32)
        osa[r * 16:(r + 1) * 16, :] = o[:, 0:128]
        osb[r * 16:(r + 1) * 16, :] = o[:, 128:256]

    s_new = [scores(0)]
    for r in range(1, DEV):
        s_new.append(scores(r))
        values(r - 1, s_new[r - 1])
    values(r, s_new[r])

    for b in CORES:
        for hh in CORES:
            hd = b * 4 + hh
            oz[b, hh, :, 0:128] = osa[pl.ds(hd, 4, stride=16), :].astype(BF16)
            oz[b, hh, :, 128:256] = osb[pl.ds(hd, 4, stride=16), :].astype(BF16)
    start([rc(oz.at[j ^ d], orr.at[j], SEND["oz"], RECV["oz"], yz=j ^ d) for d in far])
    orr.at[j][...] = oz[j]

    def activation(q):
        arrived(yr.at[q], RECV["gy"] + q)
        g = ((p3[q, 0] + r3[q, 0]) + yr[q, 0]).astype(BF16).astype(F32)
        u = ((p3[q, 1] + r3[q, 1]) + yr[q, 1]).astype(BF16).astype(F32)
        k = i * 4 + q
        a_all.at[k][...] = (g * jax.nn.sigmoid(g) * u).astype(BF16)
        rc(a_all.at[k], a_all.at[k], SEND["ay"], RECV["ay"] + q, x=i ^ 2).start()
        rc(a_all.at[k], a_all.at[k], SEND["ad"], RECV["ad"] + q // 3, x=i ^ 1).start()

    arrived(r3, RECV["g2"])
    for q in range(3):
        activation(q)

    later[2].wait()
    z_buf[...] = jnp.zeros_like(z_buf)

    def z_add(k):
        av = a_all[k]
        rows = pl.ds(pl.multiple_of(k * 256, 256), 256)
        for n in CORES:
            z_buf[n] += dot(av, wmo_v[rows, n * 256:(n + 1) * 256])

    def z_own(q, _):
        z_add(i * 4 + q)
        return 0

    def z_partner(q, _):
        z_add((i ^ 1) * 4 + q)
        return 0

    def z_far(q, _):
        k = (i ^ 2) * 4 + q
        arrived(a_all.at[k], RECV["ay"] + q)
        rc(a_all.at[k], a_all.at[k], SEND["af"], RECV["af"] + q // 3, x=i ^ 1).start()
        z_add(k)
        return 0

    def z_fwd(q, _):
        z_add((i ^ 3) * 4 + q)
        return 0

    lax.fori_loop(0, 3, z_own, 0)
    def insert(r, _):
        k_new = kn[pl.ds(r, 1), :].astype(BF16)
        v_new = vn[pl.ds(r, 1), :].astype(BF16)
        pos_r = len_ref[r]

        def chunk(t, _):
            rows = pl.ds(pl.multiple_of(t * 256, 256), 256)
            pos = t * 256 + lax.broadcasted_iota(jnp.int32, (256, 256), 0)
            ko[r, rows, :] = jnp.where(pos == pos_r, k_new, ko[r, rows, :])
            vo[r, rows, :] = jnp.where(pos == pos_r, v_new, vo[r, rows, :])
            return 0

        return lax.fori_loop(0, 16, chunk, 0)

    lax.fori_loop(0, 2, insert, 0)
    arrived(a_all.at[:3], RECV["ad"])
    lax.fori_loop(0, 3, z_partner, 0)
    activation(3)
    arrived(orr.at[:3], RECV["oz"])
    for hh in CORES:
        o_all.at[i][hh] = jnp.concatenate([orr[b, hh].astype(F32) for b in CORES], axis=0).astype(BF16)
    start([rc(o_all.at[i], o_all.at[i], SEND["ox"], RECV["ox"], x=i ^ d) for d in (2, 3, 1)])
    lax.fori_loop(3, 4, z_own, 0)
    lax.fori_loop(0, 3, z_far, 0)
    lax.fori_loop(2, 4, insert, 0)
    arrived(a_all.at[0], RECV["ad"] + 1)
    lax.fori_loop(3, 4, z_partner, 0)
    lax.fori_loop(3, 4, z_far, 0)
    arrived(a_all.at[:3], RECV["af"])
    lax.fori_loop(0, 3, z_fwd, 0)

    arrived(o_all.at[:3], RECV["ox"])
    later[3].wait()
    ov = [jnp.concatenate([o_all[b, hh] for b in CORES], axis=0) for hh in CORES]
    ov = jnp.concatenate(ov, axis=1)
    for n in CORES:
        z_buf[n] += dot(ov, wao_v[:, n * 256:(n + 1) * 256])
    arrived(a_all.at[0], RECV["af"] + 1)
    k = (i ^ 3) * 4 + 3
    rows = pl.ds(pl.multiple_of(k * 256, 256), 256)
    for d, out in enumerate((z0, z1, z2, z3)):
        cols = pl.ds(pl.multiple_of((j ^ d) * 256, 256), 256)
        out[...] = z_buf[j ^ d] + dot(a_all[k], wmo_v[rows, cols])

    for ref, s in ((st.at[:QROWS - 1], SEND["ls"]), (xg.at[:3], SEND["lx"]), (gs.at[:3], SEND["lg"]), (qr, SEND["qd"]),
                   (qys, SEND["qy"]), (zs.at[:3], SEND["qz"]), (gs0, SEND["g0"]), (ys, SEND["gy"]), (gs2, SEND["g2"]), (a_all.at[0:4], SEND["ad"]),
                   (a_all.at[0:4], SEND["ay"]), (a_all.at[0:4], SEND["af"]), (oz.at[:3], SEND["oz"]), (o_all.at[:3], SEND["ox"])):
        sent(ref, s)


def write_kernel(ki, vi, ko, vo, sem):
    copies = [pltpu.make_async_copy(ki, ko, sem.at[0]), pltpu.make_async_copy(vi, vo, sem.at[1])]
    for c in copies:
        c.start()
    for c in copies:
        c.wait()


def solution(mesh):
    both_axes = ("x", "yz")
    row_spec = P("dp", both_axes)
    in_w_spec = P("x", "yz")
    out_w_spec = P("yz", "x")
    cache_spec = P(("dp", "x", "yz"), None, None)
    len_spec = P(("dp", "x", "yz"))

    def local_layer(x_loc, gain_loc, wqkv, wg, wu, wao, wmo, kc, vc, len_loc):
        half_dim = kc.shape[2] // 2
        inv_freq = np.float32(10000.0) ** (-np.arange(half_dim, dtype=np.float32) / np.float32(half_dim))
        vm = pl.BlockSpec(memory_space=pltpu.VMEM)
        hbm = pl.BlockSpec(memory_space=pl.ANY)
        *zs, ko, vo = pl.pallas_call(
            layer_kernel, name="layer",
            out_shape=(*[pltpu.VMEM(x_loc.shape, F32)] * DEV, pltpu.VMEM(kc.shape, BF16), pltpu.VMEM(vc.shape, BF16)),
            in_specs=[hbm] * 11,
            out_specs=(vm,) * 6,
            scratch_shapes=[
                vmem(BF16, BLK), vmem(F32, 1, HALF), pltpu.SMEM((DEV,), jnp.int32),
                vmem(BF16, FF, wqkv.shape[1]), vmem(BF16, DEV, FF, FF), vmem(BF16, DEV, FF, FF),
                vmem(BF16, *wao.shape), vmem(BF16, *wmo.shape),
                vmem(BF16, DEV, ROWS, BLK), vmem(F32, DEV, 1, BLK), vmem(F32, QROWS, 1, HALF),
                vmem(F32, 2, DEV, HALF), vmem(BF16, ROWS, FF),
                vmem(F32, 3, DEV, QROWS, THIRD), vmem(F32, 2, 3, QROWS, THIRD), vmem(F32, 3, QROWS, THIRD),
                vmem(F32, 3, QROWS, THIRD), vmem(BF16, DEV, DEV, 3 * THIRD), vmem(BF16, DEV, DEV, 3 * THIRD),
                vmem(F32, HALF, HALF), vmem(F32, HALF, HALF), vmem(F32, 8, BLK), vmem(F32, 8, BLK),
                vmem(F32, DEV, QROWS, kc.shape[1]), vmem(F32, ROWS, HALF), vmem(F32, ROWS, HALF)]
            + [vmem(F32, DEV, 2, ROWS, BLK)] * 7
            + [vmem(BF16, QROWS, ROWS, BLK), vmem(BF16, DEV, DEV, DEV, BLK), vmem(BF16, DEV, DEV, DEV, BLK),
               vmem(BF16, DEV, DEV, QROWS, BLK), vmem(F32, DEV, ROWS, BLK)]
            + [pltpu.SemaphoreType.DMA((n,)) for n in (N_LOAD, N_SEND, N_RECV)],
            compiler_params=pltpu.CompilerParams(collective_id=0, has_side_effects=True,
                                                 vmem_limit_bytes=46 * 1024 * 1024),
        )(x_loc, gain_loc, inv_freq.reshape(1, -1), len_loc, wqkv, wg, wu, wao, wmo, kc, vc)
        n_yz = lax.axis_size("yz")
        parts = [lax.ppermute(zs[d], "yz", [(a, a ^ d) for a in range(n_yz)]) for d in (2, 3, 1)]
        k_out, v_out = pl.pallas_call(
            write_kernel, name="write",
            out_shape=tuple(jax.ShapeDtypeStruct(a.shape, BF16) for a in (kc, vc)),
            in_specs=[vm] * 2,
            out_specs=[hbm] * 2,
            scratch_shapes=[pltpu.SemaphoreType.DMA((2,))],
            compiler_params=pltpu.CompilerParams(vmem_limit_bytes=8 * 1024 * 1024),
            cost_estimate=pl.CostEstimate(flops=10**10, bytes_accessed=2 * kc.size * 4, transcendentals=0),
        )(ko, vo)
        y = (x_loc.astype(F32) + zs[0]) + (parts[0] + parts[1] + parts[2])
        return y.astype(BF16), k_out, v_out

    in_specs = (row_spec, P(both_axes), in_w_spec, in_w_spec, in_w_spec, out_w_spec, out_w_spec, cache_spec, cache_spec, len_spec)
    out_specs = (row_spec, cache_spec, cache_spec)
    return jax.shard_map(local_layer, mesh=mesh, in_specs=in_specs, out_specs=out_specs, check_vma=False)
```

```python
import jax
import numpy as np
import jax.numpy as jnp
from jax import lax
from jax.sharding import PartitionSpec as P
from jax.experimental import pallas as pl
from jax.experimental.pallas import tpu as pltpu

MESH = pl.DeviceIdType.MESH
F32 = jnp.float32
BF16 = jnp.bfloat16

ROWS, BLK, QROWS, DEV, THIRD, FF = 64, 256, 16, 4, 384, 1024
HALF = BLK // 2
CORES = range(DEV)
AWAY = (3, 2, 1)


def slots(*words):
    out, at = {}, 0
    for word in " ".join(words).split():
        name, _, n = word.partition("*")
        out[name] = at
        at += int(n or 1)
    return out, at


SEND, N_SEND = slots("lx lg ls", "qd qy qz g0", "gy g2 ad ay", "af oz ox z")
RECV, N_RECV = slots("lx lg ls", "q0*3 q1 qy qz", "g0*4 gy*4 g2 ad*2", "ay*4 af*2 oz ox*3", "z")
LOAD, N_LOAD = slots("x qkv gu*4 k", "v mo ao small*3")


def vmem(dtype, *shape):
    return pltpu.VMEM(shape, dtype)


def dot(a, b):
    return jnp.dot(a, b, preferred_element_type=F32)


def layer_kernel(x_hbm, g_hbm, freq_hbm, len_hbm, wqkv, wg, wu, wao, wmo, kc, vc,
                 z0, z1, z2, z3, kn, vn, ko, vo,
                 g_v, freq_v, len_ref, wqkv_v, wg_v, wu_v, wao_v, wmo_v,
                 xg, gs, st, cs, h_ref, qp, qr, qys, qy, zs, zr, qa, qb, s_ref, osa, osb,
                 gs0, r1, ys, yr, gs2, r3, p3, a_all, oz, orr, o_all, z_buf,
                 lsem, ssem, rsem):
    i = lax.axis_index("x")
    j = lax.axis_index("yz")
    d_model = 16 * x_hbm.shape[1]
    inner = (j + 1) // 2 % 2
    far = (3 - inner, 2 + inner, 1)

    def rc(src, dst, s, r, **dev):
        return pltpu.make_async_remote_copy(src_ref=src, dst_ref=dst, send_sem=ssem.at[s], recv_sem=rsem.at[r],
                                            device_id=dev, device_id_type=MESH)

    def start(copies):
        for c in copies:
            c.start()

    def arrived(ref, r):
        rc(ref, ref, 0, r, x=i ^ 1).wait_recv()

    def sent(ref, s):
        rc(ref, ref, s, 0, x=i ^ 1).wait_send()

    barrier = pltpu.get_barrier_semaphore()
    group = [(n % DEV, n // DEV) for n in range(1, QROWS)]
    for dx, dz in group:
        pl.semaphore_signal(barrier, inc=1, device_id={"x": i ^ dx, "yz": j ^ dz}, device_id_type=MESH)
    small = [pltpu.make_async_copy(x_hbm, xg.at[j], lsem.at[LOAD["x"]]),
             pltpu.make_async_copy(g_hbm, g_v, lsem.at[LOAD["small"]]),
             pltpu.make_async_copy(freq_hbm, freq_v, lsem.at[LOAD["small"] + 1]),
             pltpu.make_async_copy(len_hbm, len_ref, lsem.at[LOAD["small"] + 2])]
    start(small)
    qkv_load = pltpu.make_async_copy(wqkv, wqkv_v, lsem.at[LOAD["qkv"]])
    qkv_load.start()
    for s in CORES:
        cols = pl.ds(pl.multiple_of((i ^ (3 - s)) * 1024, 1024), 1024)
        pltpu.make_async_copy(wg.at[:, cols], wg_v.at[s], lsem.at[LOAD["gu"] + s]).start()
        pltpu.make_async_copy(wu.at[:, cols], wu_v.at[s], lsem.at[LOAD["gu"] + s]).start()

    def gu_loaded(s):
        pltpu.make_async_copy(wg_v.at[0:2], wg_v.at[0:2], lsem.at[LOAD["gu"] + s]).wait()

    later = [pltpu.make_async_copy(kc, ko, lsem.at[LOAD["k"]]), pltpu.make_async_copy(vc, vo, lsem.at[LOAD["v"]]),
             pltpu.make_async_copy(wmo, wmo_v, lsem.at[LOAD["mo"]]), pltpu.make_async_copy(wao, wao_v, lsem.at[LOAD["ao"]])]

    for c in small:
        c.wait()
    gs.at[j][...] = g_v[...].reshape(1, 256).astype(F32)
    xf = xg[j].astype(F32)
    s1 = jnp.sum(xf, axis=1, keepdims=True)
    s2 = jnp.sum(xf * xf, axis=1, keepdims=True)
    stat = jnp.broadcast_to(jnp.concatenate([s1, s2], axis=0), (128, 128))
    me = j * DEV + i
    st.at[me][...] = stat.T[0:1, :]
    pl.semaphore_wait(barrier, QROWS - 1)

    start([rc(st.at[me], st.at[me], SEND["ls"], RECV["ls"], x=i ^ dx, yz=j ^ dz) for dx, dz in reversed(group)])
    start([rc(xg.at[j], xg.at[j], SEND["lx"], RECV["lx"], yz=j ^ d) for d in far])
    start([rc(gs.at[j], gs.at[j], SEND["lg"], RECV["lg"], yz=j ^ d) for d in far])
    start(later)
    row = lax.broadcasted_iota(jnp.int32, (4, 128), 0)
    pos = jnp.zeros((4, 128), F32)
    for r in CORES:
        pos = jnp.where(row == r, len_ref[r].astype(F32), pos)
    angle = pos * freq_v[...]
    cs[0] = jnp.cos(angle)
    cs[1] = jnp.sin(angle)
    arrived(st.at[:QROWS - 1], RECV["ls"])
    arrived(gs.at[:3], RECV["lg"])
    arrived(xg.at[:3], RECV["lx"])
    tot = st[0]
    for n in range(1, QROWS):
        tot = tot + st[n]
    tot = jnp.broadcast_to(tot, (128, 128)).T
    mean = tot[0:64, 0:1] / d_model
    var = tot[64:128, 0:1] / d_model - mean * mean
    rstd = lax.rsqrt(var + 1e-6)
    for jj in CORES:
        xb = xg[jj].astype(F32)
        h_ref[:, jj * 256:(jj + 1) * 256] = ((xb - mean) * rstd * gs[jj]).astype(BF16)

    qkv_load.wait()
    for n in range(3):
        part = dot(h_ref[...], wqkv_v[:, n * 384:(n + 1) * 384])
        for b in CORES:
            qp[n, b] = part[b * 16:(b + 1) * 16, :]
        if n:
            rc(qp.at[n, i ^ 3], qr.at[0, n], SEND["qd"], RECV["q0"] + n, x=i ^ 1).start()
        else:
            rc(qp.at[n, i ^ 2], qy.at[n], SEND["qy"], RECV["qy"], x=i ^ 2).start()
            rc(qp.at[n, i ^ 3], qr.at[0, n], SEND["qd"], RECV["q0"], x=i ^ 3).start()
        rc(qp.at[n, i ^ 1], qr.at[1, n], SEND["qd"], RECV["q1"], x=i ^ 1).start()

    def gu_part(s, q):
        cols = pl.ds(pl.multiple_of(q * 256, 256), 256)
        hv = h_ref[...]
        return dot(hv, wg_v[s, :, cols]), dot(hv, wu_v[s, :, cols])

    gu_loaded(0)

    def slot0(q, _):
        g, u = gu_part(0, q)
        gs0[q, 0] = g
        gs0[q, 1] = u
        rc(gs0.at[q], r1.at[q], SEND["g0"], RECV["g0"] + q, x=i ^ 1).start()
        return 0

    lax.fori_loop(0, 2, slot0, 0)
    for n in range(1, 3):
        arrived(qr.at[0, n], RECV["q0"] + n)
        qys[n] = qp[n, i ^ 2] + qr[0, n]
        rc(qys.at[n], qy.at[n], SEND["qy"], RECV["qy"], x=i ^ 2).start()
    def slot1(q, _):
        g, u = gu_part(1, q)
        arrived(r1.at[q], RECV["g0"] + q)
        ys[q, 0] = g + r1[q, 0]
        ys[q, 1] = u + r1[q, 1]
        rc(ys.at[q], yr.at[q], SEND["gy"], RECV["gy"] + q, x=i ^ 2).start()
        return 0

    gu_loaded(1)

    def slot01(q, _):
        slot1(q, 0)
        return slot0(q + 2, 0)

    lax.fori_loop(0, 2, slot01, 0)
    lax.fori_loop(2, 3, slot1, 0)
    arrived(qr.at[1], RECV["q1"])
    arrived(qy, RECV["qy"])
    arrived(qr.at[0, 0], RECV["q0"])
    for n in range(3):
        other = qy[n] if n else qy[n] + qr[0, n]
        fin = ((qp[n, i] + qr[1, n]) + other).astype(BF16)
        for b in CORES:
            zs[b, :, n * 384:(n + 1) * 384] = fin[b * 4:(b + 1) * 4, :]
    start([rc(zs.at[j ^ d], zr.at[j], SEND["qz"], RECV["qz"], yz=j ^ d) for d in far])
    zr.at[j][...] = zs[j]
    lax.fori_loop(3, 4, slot1, 0)
    gu_loaded(2)

    def slot2(q, _):
        g, u = gu_part(2, q)
        gs2[q, 0] = g
        gs2[q, 1] = u
        rc(gs2.at[q], r3.at[q], SEND["g2"], RECV["g2"], x=i ^ 1).start()
        return 0

    lax.fori_loop(0, 4, slot2, 0)

    gu_loaded(3)

    def slot3(q, _):
        g, u = gu_part(3, q)
        p3[q, 0] = g
        p3[q, 1] = u
        return 0

    lax.fori_loop(0, 4, slot3, 0)
    arrived(zr.at[:3], RECV["qz"])

    cos_t = cs[0]
    sin_t = cs[1]

    def half(k):
        return zr[k // 9, :, (k % 9) * 128:(k % 9 + 1) * 128].astype(F32)

    def rope(k):
        u1, u2 = half(k), half(k + 1)
        return ((u1 * cos_t - u2 * sin_t).astype(BF16).astype(F32), (u2 * cos_t + u1 * sin_t).astype(BF16).astype(F32))

    for hd in range(16):
        t1, t2 = rope(2 * hd)
        qa[hd * 8:hd * 8 + 4, :] = t1
        qb[hd * 8:hd * 8 + 4, :] = t2
    t1, t2 = rope(32)
    kn[0:4, 0:128] = t1
    kn[0:4, 128:256] = t2
    vn[0:4, 0:128] = half(34)
    vn[0:4, 128:256] = half(35)
    for c in range(2):
        kn[4:8, c * HALF:(c + 1) * HALF] = pos
        vn[4:8, c * HALF:(c + 1) * HALF] = pos
    later[0].wait()
    later[1].wait()

    def scores(r):
        q_r = jnp.concatenate([qa[pl.ds(r, 16, stride=8), :], qb[pl.ds(r, 16, stride=8), :]], axis=1)
        pos_r = len_ref[r]
        qb16 = q_r.astype(BF16)
        for t in CORES:
            sc = lax.dot_general(qb16, ko[r, t * 1024:(t + 1) * 1024, :], (((1,), (1,)), ((), ())),
                                 preferred_element_type=F32) * 0.0625
            pos = t * 1024 + lax.broadcasted_iota(jnp.int32, (16, 1024), 1)
            s_ref[r, :, t * 1024:(t + 1) * 1024] = jnp.where(pos < pos_r, sc, -1e30)
        return jnp.sum(q_r * kn[r:r + 1, :], axis=1, keepdims=True) * 0.0625

    def values(r, s_new):
        sc = s_ref[r]
        top = jnp.maximum(jnp.max(sc, axis=1, keepdims=True), s_new)
        e = jnp.exp(sc - top)
        e_new = jnp.exp(s_new - top)
        inv = 1.0 / (jnp.sum(e, axis=1, keepdims=True) + e_new)
        o = (e_new * inv).astype(BF16).astype(F32) * vn[r:r + 1, :]
        o = o + dot((e * inv).astype(BF16), vo[r])
        o = o.astype(BF16).astype(F32)
        osa[r * 16:(r + 1) * 16, :] = o[:, 0:128]
        osb[r * 16:(r + 1) * 16, :] = o[:, 128:256]

    s_new = [scores(0)]
    for r in range(1, DEV):
        s_new.append(scores(r))
        values(r - 1, s_new[r - 1])
    values(r, s_new[r])

    for b in CORES:
        for hh in CORES:
            hd = b * 4 + hh
            oz[b, hh, :, 0:128] = osa[pl.ds(hd, 4, stride=16), :].astype(BF16)
            oz[b, hh, :, 128:256] = osb[pl.ds(hd, 4, stride=16), :].astype(BF16)
    start([rc(oz.at[j ^ d], orr.at[j], SEND["oz"], RECV["oz"], yz=j ^ d) for d in far])
    orr.at[j][...] = oz[j]

    def activation(q):
        arrived(yr.at[q], RECV["gy"] + q)
        g = ((p3[q, 0] + r3[q, 0]) + yr[q, 0]).astype(BF16).astype(F32)
        u = ((p3[q, 1] + r3[q, 1]) + yr[q, 1]).astype(BF16).astype(F32)
        k = i * 4 + q
        a_all.at[k][...] = (g * jax.nn.sigmoid(g) * u).astype(BF16)
        rc(a_all.at[k], a_all.at[k], SEND["ay"], RECV["ay"] + q, x=i ^ 2).start()
        if q == 3:
            @pl.when(i % 2 == 0)
            def _():
                rc(a_all.at[k], a_all.at[k], SEND["af"], RECV["af"] + 1, x=i ^ 3).start()
        rc(a_all.at[k], a_all.at[k], SEND["ad"], RECV["ad"] + q // 3, x=i ^ 1).start()

    arrived(r3, RECV["g2"])
    for q in range(3):
        activation(q)

    later[2].wait()
    z_buf[...] = jnp.zeros_like(z_buf)

    def z_add(k):
        av = a_all[k]
        rows = pl.ds(pl.multiple_of(k * 256, 256), 256)
        for n in CORES:
            z_buf[n] += dot(av, wmo_v[rows, n * 256:(n + 1) * 256])

    def z_own(q, _):
        z_add(i * 4 + q)
        return 0

    def z_partner(q, _):
        z_add((i ^ 1) * 4 + q)
        return 0

    def z_far(q, _):
        k = (i ^ 2) * 4 + q
        arrived(a_all.at[k], RECV["ay"] + q)
        rc(a_all.at[k], a_all.at[k], SEND["af"], RECV["af"], x=i ^ 1).start()
        z_add(k)
        return 0

    def z_fwd(q, _):
        z_add((i ^ 3) * 4 + q)
        return 0

    lax.fori_loop(0, 3, z_own, 0)
    arrived(a_all.at[:3], RECV["ad"])
    lax.fori_loop(0, 3, z_partner, 0)
    arrived(orr.at[:3], RECV["oz"])
    for hh in CORES:
        o_all.at[i][hh] = jnp.concatenate([orr[b, hh].astype(F32) for b in CORES], axis=0).astype(BF16)
    start([rc(o_all.at[i], o_all.at[i], SEND["ox"], RECV["ox"] + d, x=i ^ d) for d in (2, 1)])
    activation(3)
    lax.fori_loop(3, 4, z_own, 0)
    lax.fori_loop(0, 3, z_far, 0)
    arrived(o_all.at[0], RECV["ox"] + 2)
    rc(o_all.at[i ^ 2], o_all.at[i ^ 2], SEND["ox"], RECV["ox"], x=i ^ 1).start()
    arrived(a_all.at[0], RECV["ad"] + 1)
    lax.fori_loop(3, 4, z_partner, 0)
    def z_forwarded():
        arrived(a_all.at[:3], RECV["af"])
        lax.fori_loop(0, 3, z_fwd, 0)

    pl.when(i % 2 == 0)(z_forwarded)
    k = (i ^ 2) * 4 + 3
    arrived(a_all.at[k], RECV["ay"] + 3)

    @pl.when(i % 2 == 1)
    def _():
        rc(a_all.at[k], a_all.at[k], SEND["af"], RECV["af"] + 1, x=i ^ 1).start()

    z_add(k)
    pl.when(i % 2 == 1)(z_forwarded)

    for d in range(2):
        arrived(o_all.at[0], RECV["ox"] + d)
    later[3].wait()
    ov = [jnp.concatenate([o_all[b, hh] for b in CORES], axis=0) for hh in CORES]
    ov = jnp.concatenate(ov, axis=1)
    for n in CORES:
        z_buf[n] += dot(ov, wao_v[:, n * 256:(n + 1) * 256])
    arrived(a_all.at[0], RECV["af"] + 1)
    k = (i ^ 3) * 4 + 3
    rows = pl.ds(pl.multiple_of(k * 256, 256), 256)
    for d, out in enumerate((z0, z1, z2, z3)):
        cols = pl.ds(pl.multiple_of((j ^ d) * 256, 256), 256)
        out[...] = z_buf[j ^ d] + dot(a_all[k], wmo_v[rows, cols])

    for ref, s in ((st.at[:QROWS - 1], SEND["ls"]), (xg.at[:3], SEND["lx"]), (gs.at[:3], SEND["lg"]), (qr, SEND["qd"]),
                   (qys, SEND["qy"]), (zs.at[:3], SEND["qz"]), (gs0, SEND["g0"]), (ys, SEND["gy"]), (gs2, SEND["g2"]), (a_all.at[0:4], SEND["ad"]),
                   (a_all.at[0:4], SEND["ay"]), (a_all.at[0:4], SEND["af"]), (oz.at[:3], SEND["oz"]), (o_all.at[:3], SEND["ox"])):
        sent(ref, s)


def write_kernel(kn, vn, ki, vi, ko, vo, sk, sv, sem):
    caches = ((kn, ki, sk, ko, sem.at[0]), (vn, vi, sv, vo, sem.at[1]))
    step = 2 * BLK

    def chunk(n, _):
        r = n // (ki.shape[1] // step)
        t = n % (ki.shape[1] // step)
        rows = pl.ds(pl.multiple_of(t * step, step), step)
        hit = kn[pl.ds(DEV + r, 1), :].astype(jnp.int32) == t * step + lax.broadcasted_iota(jnp.int32, (step, BLK), 0)
        for new, src, mid, dst, s in caches:
            mid[r, rows, :] = jnp.where(hit, new[pl.ds(r, 1), :].astype(BF16), src[r, rows, :])
            pltpu.make_async_copy(mid.at[r, rows], dst.at[r, rows], s).start()
        return 0

    lax.fori_loop(0, ki.shape[0] * ki.shape[1] // step, chunk, 0)
    for _, _, mid, dst, s in caches:
        pltpu.make_async_copy(mid, dst, s).wait()


def solution(mesh):
    both_axes = ("x", "yz")
    row_spec = P("dp", both_axes)
    in_w_spec = P("x", "yz")
    out_w_spec = P("yz", "x")
    cache_spec = P(("dp", "x", "yz"), None, None)
    len_spec = P(("dp", "x", "yz"))

    def local_layer(x_loc, gain_loc, wqkv, wg, wu, wao, wmo, kc, vc, len_loc):
        half_dim = kc.shape[2] // 2
        inv_freq = np.float32(10000.0) ** (-np.arange(half_dim, dtype=np.float32) / np.float32(half_dim))
        vm = pl.BlockSpec(memory_space=pltpu.VMEM)
        hbm = pl.BlockSpec(memory_space=pl.ANY)
        *zs, kn, vn, ko, vo = pl.pallas_call(
            layer_kernel, name="layer",
            out_shape=(*[pltpu.VMEM(x_loc.shape, F32)] * DEV, *[pltpu.VMEM((2 * DEV, BLK), F32)] * 2, pltpu.VMEM(kc.shape, BF16), pltpu.VMEM(vc.shape, BF16)),
            in_specs=[hbm] * 11,
            out_specs=(vm,) * 8,
            scratch_shapes=[
                vmem(BF16, BLK), vmem(F32, 1, HALF), pltpu.SMEM((DEV,), jnp.int32),
                vmem(BF16, FF, wqkv.shape[1]), vmem(BF16, DEV, FF, FF), vmem(BF16, DEV, FF, FF),
                vmem(BF16, *wao.shape), vmem(BF16, *wmo.shape),
                vmem(BF16, DEV, ROWS, BLK), vmem(F32, DEV, 1, BLK), vmem(F32, QROWS, 1, HALF),
                vmem(F32, 2, DEV, HALF), vmem(BF16, ROWS, FF),
                vmem(F32, 3, DEV, QROWS, THIRD), vmem(F32, 2, 3, QROWS, THIRD), vmem(F32, 3, QROWS, THIRD),
                vmem(F32, 3, QROWS, THIRD), vmem(BF16, DEV, DEV, 3 * THIRD), vmem(BF16, DEV, DEV, 3 * THIRD),
                vmem(F32, HALF, HALF), vmem(F32, HALF, HALF),
                vmem(F32, DEV, QROWS, kc.shape[1]), vmem(F32, ROWS, HALF), vmem(F32, ROWS, HALF)]
            + [vmem(F32, DEV, 2, ROWS, BLK)] * 7
            + [vmem(BF16, QROWS, ROWS, BLK), vmem(BF16, DEV, DEV, DEV, BLK), vmem(BF16, DEV, DEV, DEV, BLK),
               vmem(BF16, DEV, DEV, QROWS, BLK), vmem(F32, DEV, ROWS, BLK)]
            + [pltpu.SemaphoreType.DMA((n,)) for n in (N_LOAD, N_SEND, N_RECV)],
            compiler_params=pltpu.CompilerParams(collective_id=0, has_side_effects=True,
                                                 vmem_limit_bytes=46 * 1024 * 1024),
        )(x_loc, gain_loc, inv_freq.reshape(1, -1), len_loc, wqkv, wg, wu, wao, wmo, kc, vc)
        n_yz = lax.axis_size("yz")
        parts = [lax.ppermute(zs[d], "yz", [(a, a ^ d) for a in range(n_yz)]) for d in (2, 3, 1)]
        k_out, v_out = pl.pallas_call(
            write_kernel, name="write",
            out_shape=tuple(jax.ShapeDtypeStruct(a.shape, BF16) for a in (kc, vc)),
            in_specs=[vm] * 4,
            out_specs=[hbm] * 2,
            scratch_shapes=[vmem(BF16, *kc.shape), vmem(BF16, *vc.shape), pltpu.SemaphoreType.DMA((2,))],
            compiler_params=pltpu.CompilerParams(vmem_limit_bytes=24 * 1024 * 1024),
            cost_estimate=pl.CostEstimate(flops=10**10, bytes_accessed=2 * kc.size * 4, transcendentals=0),
        )(kn, vn, ko, vo)
        y = (x_loc.astype(F32) + zs[0]) + (parts[0] + parts[1] + parts[2])
        return y.astype(BF16), k_out, v_out

    in_specs = (row_spec, P(both_axes), in_w_spec, in_w_spec, in_w_spec, out_w_spec, out_w_spec, cache_spec, cache_spec, len_spec)
    out_specs = (row_spec, cache_spec, cache_spec)
    return jax.shard_map(local_layer, mesh=mesh, in_specs=in_specs, out_specs=out_specs, check_vma=False)
```

```python
import jax
import numpy as np
import jax.numpy as jnp
from jax import lax
from jax.sharding import PartitionSpec as P
from jax.experimental import pallas as pl
from jax.experimental.pallas import tpu as pltpu

MESH = pl.DeviceIdType.MESH
F32 = jnp.float32
BF16 = jnp.bfloat16

ROWS, BLK, QROWS, DEV, THIRD, FF = 64, 256, 16, 4, 384, 1024
HALF = BLK // 2
CORES = range(DEV)
AWAY = (3, 2, 1)


def slots(*words):
    out, at = {}, 0
    for word in " ".join(words).split():
        name, _, n = word.partition("*")
        out[name] = at
        at += int(n or 1)
    return out, at


SEND, N_SEND = slots("lx lg ls", "qd qy qz g", "a oz")
RECV, N_RECV = slots("lx lg ls", "q0*3 q1 qy qz", "g0*4 gy*4 g2 ad*2", "ay*4 af*2 oz ox*3", "z")
LOAD, N_LOAD = slots("x qkv gu*4 k", "v mo ao small*3")


def vmem(dtype, *shape):
    return pltpu.VMEM(shape, dtype)


def dot(a, b):
    return jnp.dot(a, b, preferred_element_type=F32)


def layer_kernel(x_hbm, g_hbm, freq_hbm, len_hbm, wqkv, wg, wu, wao, wmo, kc, vc,
                 z0, z1, z2, z3, kn, vn, ko, vo,
                 g_v, freq_v, len_ref, wqkv_v, wg_v, wu_v, wao_v, wmo_v,
                 xg, gs, st, cs, h_ref, qp, qr, qys, qy, zs, zr, qa, qb, s_ref, osa, osb,
                 gs0, r1, ys, yr, gs2, r3, p3, a_all, oz, orr, o_all, z_buf,
                 lsem, ssem, rsem):
    i = lax.axis_index("x")
    j = lax.axis_index("yz")
    d_model = 16 * x_hbm.shape[1]
    inner = (j + 1) // 2 % 2
    far = (3 - inner, 2 + inner, 1)

    def rc(src, dst, s, r, **dev):
        return pltpu.make_async_remote_copy(src_ref=src, dst_ref=dst, send_sem=ssem.at[s], recv_sem=rsem.at[r],
                                            device_id=dev, device_id_type=MESH)

    def start(copies):
        for c in copies:
            c.start()

    def arrived(ref, r):
        rc(ref, ref, 0, r, x=i ^ 1).wait_recv()

    def sent(ref, s):
        rc(ref, ref, s, 0, x=i ^ 1).wait_send()

    barrier = pltpu.get_barrier_semaphore()
    group = [(n % DEV, n // DEV) for n in range(1, QROWS)]
    for dx, dz in group:
        pl.semaphore_signal(barrier, inc=1, device_id={"x": i ^ dx, "yz": j ^ dz}, device_id_type=MESH)
    small = [pltpu.make_async_copy(x_hbm, xg.at[j], lsem.at[LOAD["x"]]),
             pltpu.make_async_copy(g_hbm, g_v, lsem.at[LOAD["small"]]),
             pltpu.make_async_copy(freq_hbm, freq_v, lsem.at[LOAD["small"] + 1]),
             pltpu.make_async_copy(len_hbm, len_ref, lsem.at[LOAD["small"] + 2])]
    start(small)
    qkv_load = pltpu.make_async_copy(wqkv, wqkv_v, lsem.at[LOAD["qkv"]])
    qkv_load.start()
    for s in CORES:
        cols = pl.ds(pl.multiple_of((i ^ (3 - s)) * 1024, 1024), 1024)
        pltpu.make_async_copy(wg.at[:, cols], wg_v.at[s], lsem.at[LOAD["gu"] + s]).start()
        pltpu.make_async_copy(wu.at[:, cols], wu_v.at[s], lsem.at[LOAD["gu"] + s]).start()

    def gu_loaded(s):
        pltpu.make_async_copy(wg_v.at[0:2], wg_v.at[0:2], lsem.at[LOAD["gu"] + s]).wait()

    later = [pltpu.make_async_copy(kc, ko, lsem.at[LOAD["k"]]), pltpu.make_async_copy(vc, vo, lsem.at[LOAD["v"]]),
             pltpu.make_async_copy(wmo, wmo_v, lsem.at[LOAD["mo"]]), pltpu.make_async_copy(wao, wao_v, lsem.at[LOAD["ao"]])]

    for c in small:
        c.wait()
    gs.at[j][...] = g_v[...].reshape(1, 256).astype(F32)
    xf = xg[j].astype(F32)
    s1 = jnp.sum(xf, axis=1, keepdims=True)
    s2 = jnp.sum(xf * xf, axis=1, keepdims=True)
    stat = jnp.broadcast_to(jnp.concatenate([s1, s2], axis=0), (128, 128))
    me = j * DEV + i
    st.at[me][...] = stat.T[0:1, :]
    pl.semaphore_wait(barrier, QROWS - 1)

    start([rc(st.at[me], st.at[me], SEND["ls"], RECV["ls"], x=i ^ dx, yz=j ^ dz) for dx, dz in reversed(group)])
    start([rc(xg.at[j], xg.at[j], SEND["lx"], RECV["lx"], yz=j ^ d) for d in far])
    start([rc(gs.at[j], gs.at[j], SEND["lg"], RECV["lg"], yz=j ^ d) for d in far])
    start(later)
    row = lax.broadcasted_iota(jnp.int32, (4, 128), 0)
    pos = jnp.zeros((4, 128), F32)
    for r in CORES:
        pos = jnp.where(row == r, len_ref[r].astype(F32), pos)
    angle = pos * freq_v[...]
    cs[0] = jnp.cos(angle)
    cs[1] = jnp.sin(angle)
    arrived(st.at[:QROWS - 1], RECV["ls"])
    arrived(gs.at[:3], RECV["lg"])
    arrived(xg.at[:3], RECV["lx"])
    tot = st[0]
    for n in range(1, QROWS):
        tot = tot + st[n]
    tot = jnp.broadcast_to(tot, (128, 128)).T
    mean = tot[0:64, 0:1] / d_model
    var = tot[64:128, 0:1] / d_model - mean * mean
    rstd = lax.rsqrt(var + 1e-6)
    for jj in CORES:
        xb = xg[jj].astype(F32)
        h_ref[:, jj * 256:(jj + 1) * 256] = ((xb - mean) * rstd * gs[jj]).astype(BF16)

    qkv_load.wait()
    for n in range(3):
        part = dot(h_ref[...], wqkv_v[:, n * 384:(n + 1) * 384])
        for b in CORES:
            qp[n, b] = part[b * 16:(b + 1) * 16, :]
        if n:
            rc(qp.at[n, i ^ 3], qr.at[0, n], SEND["qd"], RECV["q0"] + n, x=i ^ 1).start()
        else:
            rc(qp.at[n, i ^ 2], qy.at[n], SEND["qy"], RECV["qy"], x=i ^ 2).start()
            rc(qp.at[n, i ^ 3], qr.at[0, n], SEND["qd"], RECV["q0"], x=i ^ 3).start()
        rc(qp.at[n, i ^ 1], qr.at[1, n], SEND["qd"], RECV["q1"], x=i ^ 1).start()

    def gu_part(s, q):
        cols = pl.ds(pl.multiple_of(q * 256, 256), 256)
        hv = h_ref[...]
        return dot(hv, wg_v[s, :, cols]), dot(hv, wu_v[s, :, cols])

    gu_loaded(0)

    def slot0(q, _):
        g, u = gu_part(0, q)
        gs0[q, 0] = g
        gs0[q, 1] = u
        rc(gs0.at[q], r1.at[q], SEND["g"], RECV["g0"] + q, x=i ^ 1).start()
        return 0

    lax.fori_loop(0, 2, slot0, 0)
    for n in range(1, 3):
        arrived(qr.at[0, n], RECV["q0"] + n)
        qys[n] = qp[n, i ^ 2] + qr[0, n]
        rc(qys.at[n], qy.at[n], SEND["qy"], RECV["qy"], x=i ^ 2).start()
    def slot1(q, _):
        g, u = gu_part(1, q)
        arrived(r1.at[q], RECV["g0"] + q)
        ys[q, 0] = g + r1[q, 0]
        ys[q, 1] = u + r1[q, 1]
        rc(ys.at[q], yr.at[q], SEND["g"], RECV["gy"] + q, x=i ^ 2).start()
        return 0

    gu_loaded(1)

    def slot01(q, _):
        slot1(q, 0)
        return slot0(q + 2, 0)

    lax.fori_loop(0, 2, slot01, 0)
    lax.fori_loop(2, 3, slot1, 0)
    arrived(qr.at[1], RECV["q1"])
    arrived(qy, RECV["qy"])
    arrived(qr.at[0, 0], RECV["q0"])
    for n in range(3):
        other = qy[n] if n else qy[n] + qr[0, n]
        fin = ((qp[n, i] + qr[1, n]) + other).astype(BF16)
        for b in CORES:
            zs[b, :, n * 384:(n + 1) * 384] = fin[b * 4:(b + 1) * 4, :]
    start([rc(zs.at[j ^ d], zr.at[j], SEND["qz"], RECV["qz"], yz=j ^ d) for d in far])
    zr.at[j][...] = zs[j]
    lax.fori_loop(3, 4, slot1, 0)
    gu_loaded(2)

    def slot2(q, _):
        g, u = gu_part(2, q)
        gs2[q, 0] = g
        gs2[q, 1] = u
        rc(gs2.at[q], r3.at[q], SEND["g"], RECV["g2"], x=i ^ 1).start()
        return 0

    lax.fori_loop(0, 4, slot2, 0)

    gu_loaded(3)

    def slot3(q, _):
        g, u = gu_part(3, q)
        p3[q, 0] = g
        p3[q, 1] = u
        return 0

    lax.fori_loop(0, 4, slot3, 0)
    arrived(zr.at[:3], RECV["qz"])

    cos_t = cs[0]
    sin_t = cs[1]

    def half(k):
        return zr[k // 9, :, (k % 9) * 128:(k % 9 + 1) * 128].astype(F32)

    def rope(k):
        u1, u2 = half(k), half(k + 1)
        return ((u1 * cos_t - u2 * sin_t).astype(BF16).astype(F32), (u2 * cos_t + u1 * sin_t).astype(BF16).astype(F32))

    for hd in range(16):
        t1, t2 = rope(2 * hd)
        qa[hd * 8:hd * 8 + 4, :] = t1
        qb[hd * 8:hd * 8 + 4, :] = t2
    t1, t2 = rope(32)
    kn[0:4, 0:128] = t1
    kn[0:4, 128:256] = t2
    vn[0:4, 0:128] = half(34)
    vn[0:4, 128:256] = half(35)
    for c in range(2):
        kn[4:8, c * HALF:(c + 1) * HALF] = pos
        vn[4:8, c * HALF:(c + 1) * HALF] = pos
    later[0].wait()
    later[1].wait()

    def scores(r):
        q_r = jnp.concatenate([qa[pl.ds(r, 16, stride=8), :], qb[pl.ds(r, 16, stride=8), :]], axis=1)
        pos_r = len_ref[r]
        qb16 = q_r.astype(BF16)
        for t in CORES:
            sc = lax.dot_general(qb16, ko[r, t * 1024:(t + 1) * 1024, :], (((1,), (1,)), ((), ())),
                                 preferred_element_type=F32) * 0.0625
            pos = t * 1024 + lax.broadcasted_iota(jnp.int32, (16, 1024), 1)
            s_ref[r, :, t * 1024:(t + 1) * 1024] = jnp.where(pos < pos_r, sc, -1e30)
        return jnp.sum(q_r * kn[r:r + 1, :], axis=1, keepdims=True) * 0.0625

    def values(r, s_new):
        sc = s_ref[r]
        top = jnp.maximum(jnp.max(sc, axis=1, keepdims=True), s_new)
        e = jnp.exp(sc - top)
        e_new = jnp.exp(s_new - top)
        inv = 1.0 / (jnp.sum(e, axis=1, keepdims=True) + e_new)
        o = (e_new * inv).astype(BF16).astype(F32) * vn[r:r + 1, :]
        o = o + dot((e * inv).astype(BF16), vo[r])
        o = o.astype(BF16).astype(F32)
        osa[r * 16:(r + 1) * 16, :] = o[:, 0:128]
        osb[r * 16:(r + 1) * 16, :] = o[:, 128:256]

    s_new = [scores(0)]
    for r in range(1, DEV):
        s_new.append(scores(r))
        values(r - 1, s_new[r - 1])
    values(r, s_new[r])

    for b in CORES:
        for hh in CORES:
            hd = b * 4 + hh
            oz[b, hh, :, 0:128] = osa[pl.ds(hd, 4, stride=16), :].astype(BF16)
            oz[b, hh, :, 128:256] = osb[pl.ds(hd, 4, stride=16), :].astype(BF16)
    start([rc(oz.at[j ^ d], orr.at[j], SEND["oz"], RECV["oz"], yz=j ^ d) for d in far])
    orr.at[j][...] = oz[j]

    def activation(q):
        arrived(yr.at[q], RECV["gy"] + q)
        g = ((p3[q, 0] + r3[q, 0]) + yr[q, 0]).astype(BF16).astype(F32)
        u = ((p3[q, 1] + r3[q, 1]) + yr[q, 1]).astype(BF16).astype(F32)
        k = i * 4 + q
        a_all.at[k][...] = (g * jax.nn.sigmoid(g) * u).astype(BF16)
        rc(a_all.at[k], a_all.at[k], SEND["a"], RECV["ay"] + q, x=i ^ 2).start()
        if q == 3:
            @pl.when(i % 2 == 0)
            def _():
                rc(a_all.at[k], a_all.at[k], SEND["a"], RECV["af"] + 1, x=i ^ 3).start()
        rc(a_all.at[k], a_all.at[k], SEND["a"], RECV["ad"] + q // 3, x=i ^ 1).start()

    arrived(r3, RECV["g2"])
    for q in range(3):
        activation(q)

    later[2].wait()
    z_buf[...] = jnp.zeros_like(z_buf)

    def z_add(k):
        av = a_all[k]
        rows = pl.ds(pl.multiple_of(k * 256, 256), 256)
        for n in CORES:
            z_buf[n] += dot(av, wmo_v[rows, n * 256:(n + 1) * 256])

    def z_own(q, _):
        z_add(i * 4 + q)
        return 0

    def z_partner(q, _):
        z_add((i ^ 1) * 4 + q)
        return 0

    def z_far(q, _):
        k = (i ^ 2) * 4 + q
        arrived(a_all.at[k], RECV["ay"] + q)
        rc(a_all.at[k], a_all.at[k], SEND["a"], RECV["af"], x=i ^ 1).start()
        z_add(k)
        return 0

    def z_fwd(q, _):
        z_add((i ^ 3) * 4 + q)
        return 0

    lax.fori_loop(0, 3, z_own, 0)
    arrived(a_all.at[:3], RECV["ad"])
    lax.fori_loop(0, 3, z_partner, 0)
    arrived(orr.at[:3], RECV["oz"])
    for hh in CORES:
        o_all.at[i][hh] = jnp.concatenate([orr[b, hh].astype(F32) for b in CORES], axis=0).astype(BF16)
    start([rc(o_all.at[i], o_all.at[i], SEND["lx"], RECV["ox"] + d, x=i ^ d) for d in (2, 1)])
    activation(3)
    lax.fori_loop(3, 4, z_own, 0)
    lax.fori_loop(0, 3, z_far, 0)
    arrived(o_all.at[0], RECV["ox"] + 2)
    rc(o_all.at[i ^ 2], o_all.at[i ^ 2], SEND["lx"], RECV["ox"], x=i ^ 1).start()
    arrived(a_all.at[0], RECV["ad"] + 1)
    lax.fori_loop(3, 4, z_partner, 0)
    def z_forwarded():
        arrived(a_all.at[:3], RECV["af"])
        lax.fori_loop(0, 3, z_fwd, 0)

    pl.when(i % 2 == 0)(z_forwarded)
    k = (i ^ 2) * 4 + 3
    arrived(a_all.at[k], RECV["ay"] + 3)

    @pl.when(i % 2 == 1)
    def _():
        rc(a_all.at[k], a_all.at[k], SEND["a"], RECV["af"] + 1, x=i ^ 1).start()

    z_add(k)
    pl.when(i % 2 == 1)(z_forwarded)

    for d in range(2):
        arrived(o_all.at[0], RECV["ox"] + d)
    later[3].wait()
    ov = [jnp.concatenate([o_all[b, hh] for b in CORES], axis=0) for hh in CORES]
    ov = jnp.concatenate(ov, axis=1)
    for n in CORES:
        z_buf[n] += dot(ov, wao_v[:, n * 256:(n + 1) * 256])
    arrived(a_all.at[0], RECV["af"] + 1)
    k = (i ^ 3) * 4 + 3
    rows = pl.ds(pl.multiple_of(k * 256, 256), 256)
    for d, out in enumerate((z0, z1, z2, z3)):
        cols = pl.ds(pl.multiple_of((j ^ d) * 256, 256), 256)
        out[...] = z_buf[j ^ d] + dot(a_all[k], wmo_v[rows, cols])

    for ref, s in ((st.at[:QROWS - 1], SEND["ls"]), (a_all.at[:6], SEND["lx"]), (gs.at[:3], SEND["lg"]), (qr, SEND["qd"]),
                   (qys, SEND["qy"]), (zs.at[:3], SEND["qz"]), (wmo_v.at[:3 * BLK], SEND["g"]),
                   (a_all.at[:12], SEND["a"]), (oz.at[:3], SEND["oz"])):
        sent(ref, s)


def write_kernel(kn, vn, ki, vi, ko, vo, sk, sv, sem):
    caches = ((kn, ki, sk, ko, sem.at[0]), (vn, vi, sv, vo, sem.at[1]))
    step = BLK

    def chunk(n, _):
        r = n // (ki.shape[1] // step)
        t = n % (ki.shape[1] // step)
        rows = pl.ds(pl.multiple_of(t * step, step), step)
        hit = kn[pl.ds(DEV + r, 1), :].astype(jnp.int32) == t * step + lax.broadcasted_iota(jnp.int32, (step, BLK), 0)
        for new, src, mid, dst, s in caches:
            mid[r, rows, :] = jnp.where(hit, new[pl.ds(r, 1), :].astype(BF16), src[r, rows, :])
            pltpu.make_async_copy(mid.at[r, rows], dst.at[r, rows], s).start()
        return 0

    lax.fori_loop(0, ki.shape[0] * ki.shape[1] // step, chunk, 0)
    for _, _, mid, dst, s in caches:
        pltpu.make_async_copy(mid, dst, s).wait()


def solution(mesh):
    both_axes = ("x", "yz")
    row_spec = P("dp", both_axes)
    in_w_spec = P("x", "yz")
    out_w_spec = P("yz", "x")
    cache_spec = P(("dp", "x", "yz"), None, None)
    len_spec = P(("dp", "x", "yz"))

    def local_layer(x_loc, gain_loc, wqkv, wg, wu, wao, wmo, kc, vc, len_loc):
        half_dim = kc.shape[2] // 2
        inv_freq = np.float32(10000.0) ** (-np.arange(half_dim, dtype=np.float32) / np.float32(half_dim))
        vm = pl.BlockSpec(memory_space=pltpu.VMEM)
        hbm = pl.BlockSpec(memory_space=pl.ANY)
        *zs, kn, vn, ko, vo = pl.pallas_call(
            layer_kernel, name="layer",
            out_shape=(*[pltpu.VMEM(x_loc.shape, F32)] * DEV, *[pltpu.VMEM((2 * DEV, BLK), F32)] * 2, pltpu.VMEM(kc.shape, BF16), pltpu.VMEM(vc.shape, BF16)),
            in_specs=[hbm] * 11,
            out_specs=(vm,) * 8,
            scratch_shapes=[
                vmem(BF16, BLK), vmem(F32, 1, HALF), pltpu.SMEM((DEV,), jnp.int32),
                vmem(BF16, FF, wqkv.shape[1]), vmem(BF16, DEV, FF, FF), vmem(BF16, DEV, FF, FF),
                vmem(BF16, *wao.shape), vmem(BF16, *wmo.shape),
                vmem(BF16, DEV, ROWS, BLK), vmem(F32, DEV, 1, BLK), vmem(F32, QROWS, 1, HALF),
                vmem(F32, 2, DEV, HALF), vmem(BF16, ROWS, FF),
                vmem(F32, 3, DEV, QROWS, THIRD), vmem(F32, 2, 3, QROWS, THIRD), vmem(F32, 3, QROWS, THIRD),
                vmem(F32, 3, QROWS, THIRD), vmem(BF16, DEV, DEV, 3 * THIRD), vmem(BF16, DEV, DEV, 3 * THIRD),
                vmem(F32, HALF, HALF), vmem(F32, HALF, HALF),
                vmem(F32, DEV, QROWS, kc.shape[1]), vmem(F32, ROWS, HALF), vmem(F32, ROWS, HALF)]
            + [vmem(F32, DEV, 2, ROWS, BLK)] * 7
            + [vmem(BF16, QROWS, ROWS, BLK), vmem(BF16, DEV, DEV, DEV, BLK), vmem(BF16, DEV, DEV, DEV, BLK),
               vmem(BF16, DEV, DEV, QROWS, BLK), vmem(F32, DEV, ROWS, BLK)]
            + [pltpu.SemaphoreType.DMA((n,)) for n in (N_LOAD, N_SEND, N_RECV)],
            compiler_params=pltpu.CompilerParams(collective_id=0, has_side_effects=True,
                                                 vmem_limit_bytes=46 * 1024 * 1024),
        )(x_loc, gain_loc, inv_freq.reshape(1, -1), len_loc, wqkv, wg, wu, wao, wmo, kc, vc)
        n_yz = lax.axis_size("yz")
        parts = [lax.ppermute(zs[d], "yz", [(a, a ^ d) for a in range(n_yz)]) for d in (2, 3, 1)]
        k_out, v_out = pl.pallas_call(
            write_kernel, name="write",
            out_shape=tuple(jax.ShapeDtypeStruct(a.shape, BF16) for a in (kc, vc)),
            in_specs=[vm] * 4,
            out_specs=[hbm] * 2,
            scratch_shapes=[vmem(BF16, *kc.shape), vmem(BF16, *vc.shape), pltpu.SemaphoreType.DMA((2,))],
            compiler_params=pltpu.CompilerParams(vmem_limit_bytes=24 * 1024 * 1024),
            cost_estimate=pl.CostEstimate(flops=10**10, bytes_accessed=2 * kc.size * 4, transcendentals=0),
        )(kn, vn, ko, vo)
        y = (x_loc.astype(F32) + zs[0]) + (parts[0] + parts[1] + parts[2])
        return y.astype(BF16), k_out, v_out

    in_specs = (row_spec, P(both_axes), in_w_spec, in_w_spec, in_w_spec, out_w_spec, out_w_spec, cache_spec, cache_spec, len_spec)
    out_specs = (row_spec, cache_spec, cache_spec)
    return jax.shard_map(local_layer, mesh=mesh, in_specs=in_specs, out_specs=out_specs, check_vma=False)
```

```python
import jax
import numpy as np
import jax.numpy as jnp
from jax import lax
from jax.sharding import PartitionSpec as P
from jax.experimental import pallas as pl
from jax.experimental.pallas import tpu as pltpu

MESH = pl.DeviceIdType.MESH
F32 = jnp.float32
BF16 = jnp.bfloat16

ROWS, BLK, QROWS, DEV, THIRD, FF = 64, 256, 16, 4, 384, 1024
HALF = BLK // 2
CORES = range(DEV)
AWAY = (3, 2, 1)


def slots(*words):
    out, at = {}, 0
    for word in " ".join(words).split():
        name, _, n = word.partition("*")
        out[name] = at
        at += int(n or 1)
    return out, at


SEND, N_SEND = slots("lx lg ls", "qd qy qz g", "a oz")
RECV, N_RECV = slots("lx lg ls", "q0*3 q1 qy qz", "g0*4 gy*4 g2 ad*2", "ay*4 af*2 oz ox*3", "z")
LOAD, N_LOAD = slots("x qkv gu*4 k", "v mo ao small*3")


def vmem(dtype, *shape):
    return pltpu.VMEM(shape, dtype)


def dot(a, b):
    return jnp.dot(a, b, preferred_element_type=F32)


def layer_kernel(x_hbm, g_hbm, freq_hbm, len_hbm, wqkv, wg, wu, wao, wmo, kc, vc,
                 z0, z1, z2, z3, kn, vn, ko, vo,
                 g_v, freq_v, len_ref, wqkv_v, wg_v, wu_v, wao_v, wmo_v,
                 xg, gs, st, cs, h_ref, qp, qr, qys, qy, zs, zr, qa, qb, s_ref, osa, osb,
                 gs0, r1, ys, yr, gs2, r3, p3, a_all, oz, orr, o_all, z_buf,
                 lsem, ssem, rsem):
    i = lax.axis_index("x")
    j = lax.axis_index("yz")
    d_model = 16 * x_hbm.shape[1]
    inner = (j + 1) // 2 % 2
    far = (3 - inner, 2 + inner, 1)

    def rc(src, dst, s, r, **dev):
        return pltpu.make_async_remote_copy(src_ref=src, dst_ref=dst, send_sem=ssem.at[s], recv_sem=rsem.at[r],
                                            device_id=dev, device_id_type=MESH)

    def start(copies):
        for c in copies:
            c.start()

    def arrived(ref, r):
        rc(ref, ref, 0, r, x=i ^ 1).wait_recv()

    def sent(ref, s):
        rc(ref, ref, s, 0, x=i ^ 1).wait_send()

    barrier = pltpu.get_barrier_semaphore()
    group = [(n % DEV, n // DEV) for n in range(1, QROWS)]
    for dx, dz in group:
        pl.semaphore_signal(barrier, inc=1, device_id={"x": i ^ dx, "yz": j ^ dz}, device_id_type=MESH)
    small = [pltpu.make_async_copy(x_hbm, xg.at[j], lsem.at[LOAD["x"]]),
             pltpu.make_async_copy(g_hbm, g_v, lsem.at[LOAD["small"]]),
             pltpu.make_async_copy(freq_hbm, freq_v, lsem.at[LOAD["small"] + 1]),
             pltpu.make_async_copy(len_hbm, len_ref, lsem.at[LOAD["small"] + 2])]
    start(small)
    qkv_load = pltpu.make_async_copy(wqkv, wqkv_v, lsem.at[LOAD["qkv"]])
    qkv_load.start()
    for s in CORES:
        cols = pl.ds(pl.multiple_of((i ^ (3 - s)) * 1024, 1024), 1024)
        pltpu.make_async_copy(wg.at[:, cols], wg_v.at[s], lsem.at[LOAD["gu"] + s]).start()
        pltpu.make_async_copy(wu.at[:, cols], wu_v.at[s], lsem.at[LOAD["gu"] + s]).start()

    def gu_loaded(s):
        pltpu.make_async_copy(wg_v.at[0:2], wg_v.at[0:2], lsem.at[LOAD["gu"] + s]).wait()

    later = [pltpu.make_async_copy(kc, ko, lsem.at[LOAD["k"]]), pltpu.make_async_copy(vc, vo, lsem.at[LOAD["v"]]),
             pltpu.make_async_copy(wmo, wmo_v, lsem.at[LOAD["mo"]]), pltpu.make_async_copy(wao, wao_v, lsem.at[LOAD["ao"]])]

    for c in small:
        c.wait()
    gs.at[j][...] = g_v[...].reshape(1, 256).astype(F32)
    xf = xg[j].astype(F32)
    s1 = jnp.sum(xf, axis=1, keepdims=True)
    s2 = jnp.sum(xf * xf, axis=1, keepdims=True)
    stat = jnp.broadcast_to(jnp.concatenate([s1, s2], axis=0), (128, 128))
    me = j * DEV + i
    st.at[me][...] = stat.T[0:1, :]
    pl.semaphore_wait(barrier, QROWS - 1)

    start([rc(st.at[me], st.at[me], SEND["ls"], RECV["ls"], x=i ^ dx, yz=j ^ dz) for dx, dz in reversed(group)])
    start([rc(xg.at[j], xg.at[j], SEND["lx"], RECV["lx"], yz=j ^ d) for d in far])
    start([rc(gs.at[j], gs.at[j], SEND["lg"], RECV["lg"], yz=j ^ d) for d in far])
    start(later)
    row = lax.broadcasted_iota(jnp.int32, (4, 128), 0)
    pos = jnp.zeros((4, 128), F32)
    for r in CORES:
        pos = jnp.where(row == r, len_ref[r].astype(F32), pos)
    angle = pos * freq_v[...]
    cs[0] = jnp.cos(angle)
    cs[1] = jnp.sin(angle)
    arrived(st.at[:QROWS - 1], RECV["ls"])
    arrived(gs.at[:3], RECV["lg"])
    arrived(xg.at[:3], RECV["lx"])
    tot = st[0]
    for n in range(1, QROWS):
        tot = tot + st[n]
    tot = jnp.broadcast_to(tot, (128, 128)).T
    mean = tot[0:64, 0:1] / d_model
    var = tot[64:128, 0:1] / d_model - mean * mean
    rstd = lax.rsqrt(var + 1e-6)
    for jj in CORES:
        xb = xg[jj].astype(F32)
        h_ref[:, jj * 256:(jj + 1) * 256] = ((xb - mean) * rstd * gs[jj]).astype(BF16)

    qkv_load.wait()
    for n in range(3):
        part = dot(h_ref[...], wqkv_v[:, n * 384:(n + 1) * 384])
        for b in CORES:
            qp[n, b] = part[b * 16:(b + 1) * 16, :]
        if n:
            rc(qp.at[n, i ^ 3], qr.at[0, n], SEND["qd"], RECV["q0"] + n, x=i ^ 1).start()
        else:
            rc(qp.at[n, i ^ 2], qy.at[n], SEND["qy"], RECV["qy"], x=i ^ 2).start()
            rc(qp.at[n, i ^ 3], qr.at[0, n], SEND["qd"], RECV["q0"], x=i ^ 3).start()
        rc(qp.at[n, i ^ 1], qr.at[1, n], SEND["qd"], RECV["q1"], x=i ^ 1).start()

    def gu_part(s, q):
        cols = pl.ds(pl.multiple_of(q * 256, 256), 256)
        hv = h_ref[...]
        return dot(hv, wg_v[s, :, cols]), dot(hv, wu_v[s, :, cols])

    gu_loaded(0)

    def slot0(q, _):
        g, u = gu_part(0, q)
        gs0[q, 0] = g
        gs0[q, 1] = u
        rc(gs0.at[q], r1.at[q], SEND["g"], RECV["g0"] + q, x=i ^ 1).start()
        return 0

    lax.fori_loop(0, 2, slot0, 0)
    for n in range(1, 3):
        arrived(qr.at[0, n], RECV["q0"] + n)
        qys[n] = qp[n, i ^ 2] + qr[0, n]
        rc(qys.at[n], qy.at[n], SEND["qy"], RECV["qy"], x=i ^ 2).start()
    def slot1(q, _):
        g, u = gu_part(1, q)
        arrived(r1.at[q], RECV["g0"] + q)
        ys[q, 0] = g + r1[q, 0]
        ys[q, 1] = u + r1[q, 1]
        rc(ys.at[q], yr.at[q], SEND["g"], RECV["gy"] + q, x=i ^ 2).start()
        return 0

    gu_loaded(1)

    def slot01(q, _):
        slot1(q, 0)
        return slot0(q + 2, 0)

    lax.fori_loop(0, 2, slot01, 0)
    lax.fori_loop(2, 3, slot1, 0)
    arrived(qr.at[1], RECV["q1"])
    arrived(qy, RECV["qy"])
    arrived(qr.at[0, 0], RECV["q0"])
    for n in range(3):
        other = qy[n] if n else qy[n] + qr[0, n]
        fin = ((qp[n, i] + qr[1, n]) + other).astype(BF16)
        for b in CORES:
            zs[b, :, n * 384:(n + 1) * 384] = fin[b * 4:(b + 1) * 4, :]
    start([rc(zs.at[j ^ d], zr.at[j], SEND["qz"], RECV["qz"], yz=j ^ d) for d in far])
    zr.at[j][...] = zs[j]
    lax.fori_loop(3, 4, slot1, 0)
    gu_loaded(2)

    def slot2(q, _):
        g, u = gu_part(2, q)
        gs2[q, 0] = g
        gs2[q, 1] = u
        rc(gs2.at[q], r3.at[q], SEND["g"], RECV["g2"], x=i ^ 1).start()
        return 0

    lax.fori_loop(0, 4, slot2, 0)

    gu_loaded(3)

    def slot3(q, _):
        g, u = gu_part(3, q)
        p3[q, 0] = g
        p3[q, 1] = u
        return 0

    lax.fori_loop(0, 4, slot3, 0)
    arrived(zr.at[:3], RECV["qz"])

    cos_t = cs[0]
    sin_t = cs[1]

    def half(k):
        return zr[k // 9, :, (k % 9) * 128:(k % 9 + 1) * 128].astype(F32)

    def rope(k):
        u1, u2 = half(k), half(k + 1)
        return ((u1 * cos_t - u2 * sin_t).astype(BF16).astype(F32), (u2 * cos_t + u1 * sin_t).astype(BF16).astype(F32))

    for hd in range(16):
        t1, t2 = rope(2 * hd)
        qa[hd * 8:hd * 8 + 4, :] = t1
        qb[hd * 8:hd * 8 + 4, :] = t2
    t1, t2 = rope(32)
    kn[0:4, 0:128] = t1
    kn[0:4, 128:256] = t2
    vn[0:4, 0:128] = half(34)
    vn[0:4, 128:256] = half(35)
    for c in range(2):
        kn[4:8, c * HALF:(c + 1) * HALF] = pos
        vn[4:8, c * HALF:(c + 1) * HALF] = pos
    later[0].wait()
    later[1].wait()

    def scores(r):
        q_r = jnp.concatenate([qa[pl.ds(r, 16, stride=8), :], qb[pl.ds(r, 16, stride=8), :]], axis=1)
        pos_r = len_ref[r]
        qb16 = q_r.astype(BF16)
        for t in CORES:
            sc = lax.dot_general(qb16, ko[r, t * 1024:(t + 1) * 1024, :], (((1,), (1,)), ((), ())),
                                 preferred_element_type=F32) * 0.0625
            pos = t * 1024 + lax.broadcasted_iota(jnp.int32, (16, 1024), 1)
            s_ref[r, :, t * 1024:(t + 1) * 1024] = jnp.where(pos < pos_r, sc, -1e30)
        return jnp.sum(q_r * kn[r:r + 1, :], axis=1, keepdims=True) * 0.0625

    def values(r, s_new):
        sc = s_ref[r]
        top = jnp.maximum(jnp.max(sc, axis=1, keepdims=True), s_new)
        e = jnp.exp(sc - top)
        e_new = jnp.exp(s_new - top)
        inv = 1.0 / (jnp.sum(e, axis=1, keepdims=True) + e_new)
        o = (e_new * inv).astype(BF16).astype(F32) * vn[r:r + 1, :]
        o = o + dot((e * inv).astype(BF16), vo[r])
        o = o.astype(BF16).astype(F32)
        osa[r * 16:(r + 1) * 16, :] = o[:, 0:128]
        osb[r * 16:(r + 1) * 16, :] = o[:, 128:256]

    s_new = [scores(0)]
    for r in range(1, DEV):
        s_new.append(scores(r))
        values(r - 1, s_new[r - 1])
    values(r, s_new[r])

    for b in CORES:
        for hh in CORES:
            hd = b * 4 + hh
            oz[b, hh, :, 0:128] = osa[pl.ds(hd, 4, stride=16), :].astype(BF16)
            oz[b, hh, :, 128:256] = osb[pl.ds(hd, 4, stride=16), :].astype(BF16)
    start([rc(oz.at[j ^ d], orr.at[j], SEND["oz"], RECV["oz"], yz=j ^ d) for d in far])
    orr.at[j][...] = oz[j]

    def activation(q):
        arrived(yr.at[q], RECV["gy"] + q)
        g = ((p3[q, 0] + r3[q, 0]) + yr[q, 0]).astype(BF16).astype(F32)
        u = ((p3[q, 1] + r3[q, 1]) + yr[q, 1]).astype(BF16).astype(F32)
        k = i * 4 + q
        a_all.at[k][...] = (g * jax.nn.sigmoid(g) * u).astype(BF16)
        rc(a_all.at[k], a_all.at[k], SEND["a"], RECV["ay"] + q, x=i ^ 2).start()
        if q == 3:
            @pl.when(i % 2 == 0)
            def _():
                rc(a_all.at[k], a_all.at[k], SEND["a"], RECV["af"] + 1, x=i ^ 3).start()
        rc(a_all.at[k], a_all.at[k], SEND["a"], RECV["ad"] + q // 3, x=i ^ 1).start()

    arrived(r3, RECV["g2"])
    for q in range(3):
        activation(q)

    later[2].wait()
    z_buf[...] = jnp.zeros_like(z_buf)

    def z_add(k):
        av = a_all[k]
        rows = pl.ds(pl.multiple_of(k * 256, 256), 256)
        for n in CORES:
            z_buf[n] += dot(av, wmo_v[rows, n * 256:(n + 1) * 256])

    def z_own(q, _):
        z_add(i * 4 + q)
        return 0

    def z_partner(q, _):
        z_add((i ^ 1) * 4 + q)
        return 0

    def z_far(q, _):
        k = (i ^ 2) * 4 + q
        arrived(a_all.at[k], RECV["ay"] + q)
        rc(a_all.at[k], a_all.at[k], SEND["a"], RECV["af"], x=i ^ 1).start()
        z_add(k)
        return 0

    def z_fwd(q, _):
        z_add((i ^ 3) * 4 + q)
        return 0

    lax.fori_loop(0, 3, z_own, 0)
    arrived(a_all.at[:3], RECV["ad"])
    lax.fori_loop(0, 3, z_partner, 0)
    arrived(orr.at[:3], RECV["oz"])
    for hh in CORES:
        o_all.at[i][hh] = jnp.concatenate([orr[b, hh].astype(F32) for b in CORES], axis=0).astype(BF16)
    start([rc(o_all.at[i], o_all.at[i], SEND["lx"], RECV["ox"] + d, x=i ^ d) for d in (2, 1)])
    activation(3)
    lax.fori_loop(3, 4, z_own, 0)
    lax.fori_loop(0, 3, z_far, 0)
    arrived(o_all.at[0], RECV["ox"] + 2)
    rc(o_all.at[i ^ 2], o_all.at[i ^ 2], SEND["lx"], RECV["ox"], x=i ^ 1).start()
    arrived(a_all.at[0], RECV["ad"] + 1)
    lax.fori_loop(3, 4, z_partner, 0)
    def z_forwarded():
        arrived(a_all.at[:3], RECV["af"])
        lax.fori_loop(0, 3, z_fwd, 0)

    def z_rest():
        z_forwarded()
        for d in range(2):
            arrived(o_all.at[0], RECV["ox"] + d)
        later[3].wait()
        ov = [jnp.concatenate([o_all[b, hh] for b in CORES], axis=0) for hh in CORES]
        ov = jnp.concatenate(ov, axis=1)
        for n in CORES:
            z_buf[n] += dot(ov, wao_v[:, n * 256:(n + 1) * 256])

    pl.when(i % 2 == 0)(z_rest)
    k = (i ^ 2) * 4 + 3
    arrived(a_all.at[k], RECV["ay"] + 3)

    @pl.when(i % 2 == 1)
    def _():
        rc(a_all.at[k], a_all.at[k], SEND["a"], RECV["af"] + 1, x=i ^ 1).start()

    z_add(k)
    pl.when(i % 2 == 1)(z_rest)

    arrived(a_all.at[0], RECV["af"] + 1)
    k = (i ^ 3) * 4 + 3
    rows = pl.ds(pl.multiple_of(k * 256, 256), 256)
    for d, out in enumerate((z0, z1, z2, z3)):
        cols = pl.ds(pl.multiple_of((j ^ d) * 256, 256), 256)
        out[...] = z_buf[j ^ d] + dot(a_all[k], wmo_v[rows, cols])

    for ref, s in ((st.at[:QROWS - 1], SEND["ls"]), (a_all.at[:6], SEND["lx"]), (gs.at[:3], SEND["lg"]), (qr, SEND["qd"]),
                   (qys, SEND["qy"]), (zs.at[:3], SEND["qz"]), (wmo_v.at[:3 * BLK], SEND["g"]),
                   (a_all.at[:12], SEND["a"]), (oz.at[:3], SEND["oz"])):
        sent(ref, s)


def write_kernel(kn, vn, ki, vi, ko, vo, sk, sv, sem):
    caches = ((kn, ki, sk, ko, sem.at[0]), (vn, vi, sv, vo, sem.at[1]))
    step = BLK

    def chunk(n, _):
        r = n // (ki.shape[1] // step)
        t = n % (ki.shape[1] // step)
        rows = pl.ds(pl.multiple_of(t * step, step), step)
        hit = kn[pl.ds(DEV + r, 1), :].astype(jnp.int32) == t * step + lax.broadcasted_iota(jnp.int32, (step, BLK), 0)
        for new, src, mid, dst, s in caches:
            mid[r, rows, :] = jnp.where(hit, new[pl.ds(r, 1), :].astype(BF16), src[r, rows, :])
            pltpu.make_async_copy(mid.at[r, rows], dst.at[r, rows], s).start()
        return 0

    lax.fori_loop(0, ki.shape[0] * ki.shape[1] // step, chunk, 0)
    for _, _, mid, dst, s in caches:
        pltpu.make_async_copy(mid, dst, s).wait()


def solution(mesh):
    both_axes = ("x", "yz")
    row_spec = P("dp", both_axes)
    in_w_spec = P("x", "yz")
    out_w_spec = P("yz", "x")
    cache_spec = P(("dp", "x", "yz"), None, None)
    len_spec = P(("dp", "x", "yz"))

    def local_layer(x_loc, gain_loc, wqkv, wg, wu, wao, wmo, kc, vc, len_loc):
        half_dim = kc.shape[2] // 2
        inv_freq = np.float32(10000.0) ** (-np.arange(half_dim, dtype=np.float32) / np.float32(half_dim))
        vm = pl.BlockSpec(memory_space=pltpu.VMEM)
        hbm = pl.BlockSpec(memory_space=pl.ANY)
        *zs, kn, vn, ko, vo = pl.pallas_call(
            layer_kernel, name="layer",
            out_shape=(*[pltpu.VMEM(x_loc.shape, F32)] * DEV, *[pltpu.VMEM((2 * DEV, BLK), F32)] * 2, pltpu.VMEM(kc.shape, BF16), pltpu.VMEM(vc.shape, BF16)),
            in_specs=[hbm] * 11,
            out_specs=(vm,) * 8,
            scratch_shapes=[
                vmem(BF16, BLK), vmem(F32, 1, HALF), pltpu.SMEM((DEV,), jnp.int32),
                vmem(BF16, FF, wqkv.shape[1]), vmem(BF16, DEV, FF, FF), vmem(BF16, DEV, FF, FF),
                vmem(BF16, *wao.shape), vmem(BF16, *wmo.shape),
                vmem(BF16, DEV, ROWS, BLK), vmem(F32, DEV, 1, BLK), vmem(F32, QROWS, 1, HALF),
                vmem(F32, 2, DEV, HALF), vmem(BF16, ROWS, FF),
                vmem(F32, 3, DEV, QROWS, THIRD), vmem(F32, 2, 3, QROWS, THIRD), vmem(F32, 3, QROWS, THIRD),
                vmem(F32, 3, QROWS, THIRD), vmem(BF16, DEV, DEV, 3 * THIRD), vmem(BF16, DEV, DEV, 3 * THIRD),
                vmem(F32, HALF, HALF), vmem(F32, HALF, HALF),
                vmem(F32, DEV, QROWS, kc.shape[1]), vmem(F32, ROWS, HALF), vmem(F32, ROWS, HALF)]
            + [vmem(F32, DEV, 2, ROWS, BLK)] * 7
            + [vmem(BF16, QROWS, ROWS, BLK), vmem(BF16, DEV, DEV, DEV, BLK), vmem(BF16, DEV, DEV, DEV, BLK),
               vmem(BF16, DEV, DEV, QROWS, BLK), vmem(F32, DEV, ROWS, BLK)]
            + [pltpu.SemaphoreType.DMA((n,)) for n in (N_LOAD, N_SEND, N_RECV)],
            compiler_params=pltpu.CompilerParams(collective_id=0, has_side_effects=True,
                                                 vmem_limit_bytes=46 * 1024 * 1024),
        )(x_loc, gain_loc, inv_freq.reshape(1, -1), len_loc, wqkv, wg, wu, wao, wmo, kc, vc)
        n_yz = lax.axis_size("yz")
        parts = [lax.ppermute(zs[d], "yz", [(a, a ^ d) for a in range(n_yz)]) for d in (2, 3, 1)]
        k_out, v_out = pl.pallas_call(
            write_kernel, name="write",
            out_shape=tuple(jax.ShapeDtypeStruct(a.shape, BF16) for a in (kc, vc)),
            in_specs=[vm] * 4,
            out_specs=[hbm] * 2,
            scratch_shapes=[vmem(BF16, *kc.shape), vmem(BF16, *vc.shape), pltpu.SemaphoreType.DMA((2,))],
            compiler_params=pltpu.CompilerParams(vmem_limit_bytes=24 * 1024 * 1024),
            cost_estimate=pl.CostEstimate(flops=10**10, bytes_accessed=2 * kc.size * 4, transcendentals=0),
        )(kn, vn, ko, vo)
        y = (x_loc.astype(F32) + zs[0]) + (parts[0] + parts[1] + parts[2])
        return y.astype(BF16), k_out, v_out

    in_specs = (row_spec, P(both_axes), in_w_spec, in_w_spec, in_w_spec, out_w_spec, out_w_spec, cache_spec, cache_spec, len_spec)
    out_specs = (row_spec, cache_spec, cache_spec)
    return jax.shard_map(local_layer, mesh=mesh, in_specs=in_specs, out_specs=out_specs, check_vma=False)
```
